32 devices in a mesh: az: 4 (over y, x), rad: 8 (over z, core).
Axes of the slice: x: 2, y: 2, z: 4, core: 2. Of those that a mesh axis runs over, the one named last changes fastest.
Arguments:
- fields: float32 [5, 96, 32, 512], P(None, 'rad', None, 'az'), may hold values from -6 to 6
- shift: int32 [96], replicated, may hold values from 0 to 511
- fraction: float32 [96], replicated, may hold values from -0.5 to 0.5
- radial_rate: float32 [96, 32], replicated, may hold values from -0.4 to 0.4
Outputs:
- updated: float32 [5, 96, 32, 512], P(None, 'rad', None, 'az')
The draws below stay inside these ranges and needn't reach their ends.
All inputs are finite; a program needn't handle non-finite values.
Results may differ from the reference program's by a relative error of at most 0.0003.
Values sent between devices are 32-bit elements; how exact they have to be, the bound alone decides.
A program may use at most 64 MiB of HBM per device.

```python
import jax
import jax.numpy as jnp
from jax import lax

NP = 32
NF = 5
NA = 512
NR = 96


def touch_ends(entries, rng, low, largest):
    extent = entries.shape
    index_at = [jax.random.randint(jax.random.fold_in(rng, axis), (), 0, extent[axis]) for axis in range(len(extent))]
    entries = entries.at[tuple(index_at)].set(low)
    longest = extent.index(max(extent))
    index_at[longest] = (index_at[longest] + 1) % extent[longest]
    return entries.at[tuple(index_at)].set(largest)


def level_of(key, shape, cuts, low, high):
    level, own = 1.0, jax.random.fold_in(key, 6)
    for dim, shards_of in cuts:
        steps = jnp.exp(jax.random.uniform(jax.random.fold_in(own, dim), (shards_of,), jnp.float32, low / len(cuts), high / len(cuts)))
        level = level * jnp.repeat(steps, shape[dim] // shards_of).reshape([-1 if axis == dim else 1 for axis in range(len(shape))])
    return level


def gaussian(key, dims, scale, reach, pieces=(), kind=jnp.bfloat16):
    entries = scale * jax.random.normal(key, dims, jnp.float32)
    if pieces:
        entries = entries * level_of(key, dims, pieces, -0.22, 0.18)
    return jnp.clip(entries, -reach, reach).astype(kind)


def setup_inputs(seed: int = 0) -> dict:
    splits = jax.random.split(jax.random.key(seed), 5)
    fields = gaussian(splits[0], (NF, NR, NP, NA), 1.0, 6.0, ((1, 8), (3, 4)), jnp.float32)
    shift = touch_ends(jax.random.randint(splits[1], (NR,), 0, NA), jax.random.fold_in(splits[1], 1), 0, NA - 1).astype(jnp.int32)
    fraction = jnp.clip(jax.random.uniform(splits[2], (NR,), jnp.float32, -0.5, 0.5), -0.5, 0.5)
    radial_rate = jnp.clip(jax.random.uniform(splits[3], (NR, NP), jnp.float32, -0.4, 0.4), -0.4, 0.4)
    return {"fields": fields, "shift": shift, "fraction": fraction, "radial_rate": radial_rate}


def cut(values, low, count, axis):
    return lax.slice_in_dim(values, low, low + count, axis=axis)


def limited(left, right):
    steep = jnp.minimum(jnp.minimum(2.0 * jnp.abs(left), 2.0 * jnp.abs(right)), 0.5 * jnp.abs(left + right))
    return jnp.where(left * right > 0.0, jnp.sign(left) * steep, 0.0)


def flux_change(padded, courant, axis):
    count = padded.shape[axis] - 4
    left = cut(padded, 1, count + 2, axis) - cut(padded, 0, count + 2, axis)
    right = cut(padded, 2, count + 2, axis) - cut(padded, 1, count + 2, axis)
    slope = limited(left, right)
    forward = cut(padded, 1, count + 1, axis) + 0.5 * (1.0 - courant) * cut(slope, 0, count + 1, axis)
    backward = cut(padded, 2, count + 1, axis) - 0.5 * (1.0 + courant) * cut(slope, 1, count + 1, axis)
    flux = courant * jnp.where(courant > 0.0, forward, backward)
    return cut(flux, 1, count, axis) - cut(flux, 0, count, axis)


def one_field(single, shift, fraction, face_rates):
    rolled = lax.map(lambda item: jnp.roll(item[0], item[1], axis=-1), (single, shift))
    padded = jnp.concatenate([rolled[:, :, -2:], rolled, rolled[:, :, :2]], axis=2)
    azimuthal = rolled - flux_change(padded, fraction[:, None, None], 2)
    zeros = jnp.zeros((2,) + azimuthal.shape[1:], jnp.float32)
    radial = jnp.concatenate([zeros, azimuthal, zeros], axis=0)
    return azimuthal - flux_change(radial, face_rates[:, :, None], 0)


def reference(fields, shift, fraction, radial_rate):
    edge = jnp.zeros((1, radial_rate.shape[1]), jnp.float32)
    face_rates = jnp.concatenate([edge, radial_rate[:-1], edge], axis=0)
    return lax.map(lambda single: one_field(single, shift, fraction, face_rates), fields)
```

```python
import functools

import jax
import jax.numpy as jnp
from jax import lax
from jax.experimental import pallas as pl
from jax.experimental.pallas import tpu as pltpu
from jax.sharding import PartitionSpec as P

MESH = pl.DeviceIdType.MESH


def half_slope(left, right):
    low = jnp.maximum(jnp.minimum(left, right), 0.0)
    high = jnp.minimum(jnp.maximum(left, right), 0.0)
    return jnp.maximum(jnp.minimum(0.25 * (left + right), low), high)


def chunks_of(fields, rows, group):
    rest = rows // group - 1
    if rest == 0:
        return [(True, f, 1) for f in range(fields)]
    return [(True, 0, fields), (False, 0, fields - 2), (False, fields - 2, 2)]


def peers_of(group, me):
    if group == 4:
        inner = me + 1 - 2 * lax.rem(me, 2)
        outer = lax.rem(me + 2, 4)
        return [inner, outer], [inner + outer - me]
    return [lax.rem(me + step, group) for step in range(1, group)], []


def kernel(
    group, rings, chunks,
    fields, shift_in, fraction_in, rates_in,
    out,
    own, landed, rate, bend, shift, fraction, rates, *rest,
):
    count = len(chunks)
    gathered, results = rest[:count], rest[count : 2 * count]
    small_sem, in_sem, own_sem, send1, recv1, send2, recv2, ghost_send, ghost_recv, passed, from_above, from_below, clear = rest[2 * count :]
    nf, rows, polar, width = fields.shape
    me, ring = lax.axis_index("az"), lax.axis_index("rad")
    more = rows // group - 1
    start = ring * rows

    def base(first, d):
        if first:
            return jnp.where(d < 2, d, jnp.where(d < 4, rows - 4 + d, d - 2))
        return group - 2 + d * more

    def height(first):
        return 1 if first else more

    near, far = peers_of(group, me)
    barrier = pltpu.get_barrier_semaphore()
    for d in near:
        pl.semaphore_signal(barrier, inc=1, device_id=(d, ring), device_id_type=MESH)

    below, above = ring > 0, ring < rings - 1
    leads = me == 0

    def tell(who, semaphore, step):
        @pl.when(who)
        def _():
            pl.semaphore_signal(semaphore, inc=1, device_id=(me, ring + step), device_id_type=MESH)

    lowers, lifts = jnp.logical_and(leads, below), jnp.logical_and(leads, above)
    tell(lifts, barrier, 1)

    stages = [
        pltpu.make_async_copy(fields.at[:, pl.ds(0, group - 2)], own.at[:, pl.ds(0, group - 2)], in_sem.at[0]),
        pltpu.make_async_copy(fields.at[:, pl.ds(rows - 2, 2)], own.at[:, pl.ds(rows - 2, 2)], in_sem.at[1]),
    ]
    if more:
        stages.append(
            pltpu.make_async_copy(
                fields.at[:, pl.ds(group - 2, rows - group)],
                own.at[:, pl.ds(group - 2, rows - group)],
                in_sem.at[2],
            )
        )
    for copy in stages:
        copy.start()
    mine = []
    for c, (first, f0, n) in enumerate(chunks):
        copy = pltpu.make_async_copy(
            fields.at[pl.ds(f0, n), pl.ds(base(first, me), height(first))],
            gathered[c].at[me],
            own_sem.at[c],
        )
        copy.start()
        mine.append(copy)

    small = [
        pltpu.make_async_copy(rates_in, rates, small_sem.at[0]),
        pltpu.make_async_copy(shift_in, shift, small_sem.at[1]),
        pltpu.make_async_copy(fraction_in, fraction, small_sem.at[2]),
    ]
    for copy in small:
        copy.start()

    with jax.named_scope("barrier"):
        pl.semaphore_wait(barrier, len(near) + jnp.where(lowers, 1, 0))
    if far:
        pl.semaphore_signal(passed, inc=1, device_id=(near[0], ring), device_id_type=MESH)

    def out_copy(c, d):
        first, f0, n = chunks[c]
        return pltpu.make_async_remote_copy(
            src_ref=own.at[pl.ds(f0, n), pl.ds(base(first, d), height(first))],
            dst_ref=gathered[c].at[me],
            send_sem=send1.at[c, d],
            recv_sem=recv1.at[c, me],
            device_id=(d, ring),
            device_id_type=MESH,
        )

    def in_copy(c, s):
        first, f0, n = chunks[c]
        return pltpu.make_async_remote_copy(
            src_ref=gathered[c].at[s],
            dst_ref=gathered[c].at[s],
            send_sem=send1.at[c, s],
            recv_sem=recv1.at[c, s],
            device_id=(s, ring),
            device_id_type=MESH,
        )

    def back_copy(c, d):
        first, f0, n = chunks[c]
        return pltpu.make_async_remote_copy(
            src_ref=results[c].at[d],
            dst_ref=landed.at[pl.ds(f0, n), pl.ds(2 + base(first, me), height(first))],
            send_sem=send2.at[c, d],
            recv_sem=recv2.at[c, me],
            device_id=(d, ring),
            device_id_type=MESH,
        )

    def home_copy(c, s):
        first, f0, n = chunks[c]
        target = landed.at[pl.ds(f0, n), pl.ds(2 + base(first, s), height(first))]
        return pltpu.make_async_remote_copy(
            src_ref=target,
            dst_ref=target,
            send_sem=send2.at[c, s],
            recv_sem=recv2.at[c, s],
            device_id=(s, ring),
            device_id_type=MESH,
        )

    def peers():
        return far + near

    def ready(c):
        if c == 0:
            stages[0].wait()
            stages[1].wait()
        if c == 1 and more:
            stages[2].wait()

    for c in range(min(2, count)):
        ready(c)
        for d in near:
            out_copy(c, d).start()
    if far:
        with jax.named_scope("passed"):
            pl.semaphore_wait(passed, 1)
    tell(lowers, from_above, -1)
    for c in range(count):
        for d in far:
            out_copy(c, d).start()
        if c > 1:
            for d in near:
                out_copy(c, d).start()

    small[0].wait()
    table = rates[...]
    place = lax.broadcasted_iota(jnp.int32, table.shape, 1)
    for j in range(rows + 1):
        column = jnp.sum(
            jnp.where(place == start - 1 + j, table, 0.0), axis=1, keepdims=True
        )
        if j == 0:
            column = jnp.where(ring > 0, column, 0.0)
        if j == rows:
            column = jnp.where(ring < rings - 1, column, 0.0)
        spread = jnp.broadcast_to(column, (polar, width))
        size = jnp.abs(spread)
        rate[j] = spread
        bend[j] = size * (1.0 - size)

    @pl.when(ring == 0)
    def _():
        landed[:, 0:2] = jnp.zeros((nf, 2, polar, width), jnp.float32)

    @pl.when(ring == rings - 1)
    def _():
        landed[:, rows + 2 : rows + 4] = jnp.zeros((nf, 2, polar, width), jnp.float32)

    lane = lax.broadcasted_iota(jnp.int32, (polar, width), 1)
    at_first, at_last = lane == 0, lane == width - 1

    def previous(blocks):
        turned = [pltpu.roll(b, 1, 1) for b in blocks]
        return [jnp.where(at_first, turned[p - 1], turned[p]) for p in range(group)]

    def following(blocks):
        turned = [pltpu.roll(b, width - 1, 1) for b in blocks]
        return [jnp.where(at_last, turned[(p + 1) % group], turned[p]) for p in range(group)]

    cycle = group * width

    def azimuth(c):
        first, f0, n = chunks[c]
        source, target = gathered[c], results[c]
        for k in range(height(first)):
            row = start + base(first, me) + k
            courant = fraction[row]
            ahead = courant > 0.0
            amount = shift[row] + jnp.where(ahead, cycle, cycle - 1)
            whole = lax.rem(amount // width, group)
            part = lax.rem(amount, width)
            size = jnp.abs(courant)
            bent = size * (1.0 - size)
            beyond = lane >= part

            for f in range(n):
                turned = [
                    pltpu.roll(source[lax.rem(p + group - whole, group), f, k], part, 1)
                    for p in range(group)
                ]
                q = [jnp.where(beyond, turned[p], turned[p - 1]) for p in range(group)]
                before = previous(q)
                left = [x - y for x, y in zip(q, before)]
                right = following(left)
                value = [
                    courant * x + bent * half_slope(l, r) for x, l, r in zip(q, left, right)
                ]
                lower = previous(value)
                for p in range(group):
                    kept = jnp.where(ahead, q[p], before[p])
                    target[p, f, k] = kept - (value[p] - lower[p])
        landed[pl.ds(f0, n), pl.ds(2 + base(first, me), height(first))] = target[me]

    ghosts = [
        pltpu.make_async_remote_copy(
            src_ref=landed.at[:, pl.ds(2, 2)],
            dst_ref=landed.at[:, pl.ds(rows + 2, 2)],
            send_sem=ghost_send.at[0],
            recv_sem=ghost_recv.at[0],
            device_id=(me, jnp.maximum(ring - 1, 0)),
            device_id_type=MESH,
        ),
        pltpu.make_async_remote_copy(
            src_ref=landed.at[:, pl.ds(rows, 2)],
            dst_ref=landed.at[:, pl.ds(0, 2)],
            send_sem=ghost_send.at[1],
            recv_sem=ghost_recv.at[1],
            device_id=(me, jnp.minimum(ring + 1, rings - 1)),
            device_id_type=MESH,
        ),
    ]

    def radial(f):
        def cell(i):
            return landed[f, i]

        q1, q2 = cell(1), cell(2)
        d1 = q1 - cell(0)
        d2 = q2 - q1
        h1 = half_slope(d1, d2)
        below = None
        for j in range(rows + 1):
            q3 = cell(j + 3)
            d3 = q3 - q2
            h2 = half_slope(d2, d3)
            c, b = rate[j], bend[j]
            ahead = c > 0.0
            flux = c * jnp.where(ahead, q1, q2) + b * jnp.where(ahead, h1, h2)
            if j > 0:
                out[f, j - 1] = q1 - (flux - below)
            below = flux
            q1, q2, d2, h1 = q2, q3, d3, h2

    edges = 1 if more else count

    small[1].wait()
    small[2].wait()

    @pl.when(lifts)
    def _():
        pl.semaphore_wait(from_above, 1)

    tell(lifts, from_below, 1)
    for c in range(count):
        with jax.named_scope("arrived"):
            mine[c].wait()
            for s in peers():
                in_copy(c, s).wait_recv()
        with jax.named_scope("azimuth"):
            azimuth(c)
        for d in peers():
            back_copy(c, d).start()
        if c == 0:

            @pl.when(lowers)
            def _():
                pl.semaphore_wait(from_below, 1)

            @pl.when(leads)
            def _():
                for d in peers():
                    pl.semaphore_signal(clear, inc=1, device_id=(d, ring), device_id_type=MESH)

    @pl.when(jnp.logical_not(leads))
    def _():
        pl.semaphore_wait(clear, 1)

    with jax.named_scope("home"):
        for c in range(edges):
            for s in peers():
                home_copy(c, s).wait_recv()

    @pl.when(ring > 0)
    def _():
        ghosts[0].start()

    @pl.when(ring < rings - 1)
    def _():
        ghosts[1].start()

    @pl.when(ring > 0)
    def _():
        ghosts[1].wait_recv()

    @pl.when(ring < rings - 1)
    def _():
        ghosts[0].wait_recv()

    for c in range(edges, count):
        first, f0, n = chunks[c]
        with jax.named_scope("home"):
            for s in peers():
                home_copy(c, s).wait_recv()
        with jax.named_scope("radial"):
            for f in range(f0, f0 + n):
                radial(f)
    if not more:
        for f in range(nf):
            radial(f)

    for c in range(count):
        for d in peers():
            out_copy(c, d).wait_send()
            back_copy(c, d).wait_send()

    @pl.when(ring > 0)
    def _():
        ghosts[0].wait_send()

    @pl.when(ring < rings - 1)
    def _():
        ghosts[1].wait_send()


def shards(fields, shift, fraction, radial_rate):
    nf, rows, polar, width = fields.shape
    group, rings = lax.axis_size("az"), lax.axis_size("rad")
    chunks = chunks_of(nf, rows, group)
    more = rows // group - 1
    boxes = [
        pltpu.VMEM((group, n, 1 if first else more, polar, width), jnp.float32)
        for first, f0, n in chunks
    ]
    count = len(chunks)
    dma = pltpu.SemaphoreType.DMA
    operands = (fields, shift, fraction, radial_rate.T)
    return pl.pallas_call(
        functools.partial(kernel, group, rings, chunks),
        out_shape=jax.ShapeDtypeStruct(fields.shape, jnp.float32),
        in_specs=[pl.BlockSpec(memory_space=pltpu.HBM)] * 4,
        out_specs=pl.BlockSpec(memory_space=pltpu.VMEM),
        scratch_shapes=[
            pltpu.VMEM((nf, rows, polar, width), jnp.float32),
            pltpu.VMEM((nf, rows + 4, polar, width), jnp.float32),
            pltpu.VMEM((rows + 1, polar, width), jnp.float32),
            pltpu.VMEM((rows + 1, polar, width), jnp.float32),
            pltpu.SMEM(shift.shape, jnp.int32),
            pltpu.SMEM(fraction.shape, jnp.float32),
            pltpu.VMEM(radial_rate.shape[::-1], jnp.float32),
            *boxes,
            *boxes,
            dma((3,)),
            dma((3,)),
            dma((count,)),
            dma((count, group)),
            dma((count, group)),
            dma((count, group)),
            dma((count, group)),
            dma((2,)),
            dma((2,)),
            *[pltpu.SemaphoreType.REGULAR] * 4,
        ],
        compiler_params=pltpu.CompilerParams(
            collective_id=0, has_side_effects=True, vmem_limit_bytes=10 * fields.size * 4
        ),
    )(*(pltpu.with_memory_space_constraint(x, pltpu.HBM) for x in operands))


def solution(mesh):
    placed = (P(None, "rad", None, "az"), P(), P(), P())
    return jax.shard_map(
        shards, mesh=mesh, in_specs=placed, out_specs=P(None, "rad", None, "az"), check_vma=False
    )
```

```python
import functools

import jax
import jax.numpy as jnp
from jax import lax
from jax.experimental import pallas as pl
from jax.experimental.pallas import tpu as pltpu
from jax.sharding import PartitionSpec as P

MESH = pl.DeviceIdType.MESH


def half_slope(left, right):
    low = jnp.maximum(jnp.minimum(left, right), 0.0)
    high = jnp.minimum(jnp.maximum(left, right), 0.0)
    return jnp.maximum(jnp.minimum(0.25 * (left + right), low), high)


def chunks_of(fields, rows, group):
    rest = rows // group - 1
    if rest == 0:
        return [(True, f, 1) for f in range(fields)]
    return [(True, 0, fields), (False, 0, fields - 2), (False, fields - 2, 2)]


def peers_of(group, me):
    if group == 4:
        inner = me + 1 - 2 * lax.rem(me, 2)
        outer = lax.rem(me + 2, 4)
        return [inner, outer], [inner + outer - me]
    return [lax.rem(me + step, group) for step in range(1, group)], []


def kernel(
    group, rings, chunks,
    fields, shift_in, fraction_in, rates_in,
    out,
    own, landed, rate, bend, shift, fraction, rates, *rest,
):
    count = len(chunks)
    gathered, results = rest[:count], rest[count : 2 * count]
    small_sem, in_sem, sent, gather_sem, home_sem, ghost_send, ghost_recv, passed, told, from_below = rest[2 * count :]
    nf, rows, polar, width = fields.shape
    me, ring = lax.axis_index("az"), lax.axis_index("rad")
    more = rows // group - 1
    start = ring * rows

    def base(first, d):
        if first:
            return jnp.where(d < 2, d, jnp.where(d < 4, rows - 4 + d, d - 2))
        return group - 2 + d * more

    def height(first):
        return 1 if first else more

    near, far = peers_of(group, me)
    barrier = pltpu.get_barrier_semaphore()
    for d in near:
        pl.semaphore_signal(barrier, inc=1, device_id=(d, ring), device_id_type=MESH)

    below, above = ring > 0, ring < rings - 1
    leads = me == 0

    def tell(who, semaphore, step):
        @pl.when(who)
        def _():
            pl.semaphore_signal(semaphore, inc=1, device_id=(me, ring + step), device_id_type=MESH)

    lowers, lifts = jnp.logical_and(leads, below), jnp.logical_and(leads, above)
    tell(lifts, barrier, 1)

    stages = [
        pltpu.make_async_copy(fields.at[:, pl.ds(0, group - 2)], own.at[:, pl.ds(0, group - 2)], in_sem.at[0]),
        pltpu.make_async_copy(fields.at[:, pl.ds(rows - 2, 2)], own.at[:, pl.ds(rows - 2, 2)], in_sem.at[0]),
    ]
    if more:
        stages.append(
            pltpu.make_async_copy(
                fields.at[:, pl.ds(group - 2, rows - group)],
                own.at[:, pl.ds(group - 2, rows - group)],
                in_sem.at[1],
            )
        )
    for copy in stages:
        copy.start()
    for c, (first, f0, n) in enumerate(chunks):
        pltpu.make_async_copy(
            fields.at[pl.ds(f0, n), pl.ds(base(first, me), height(first))],
            gathered[c].at[me],
            gather_sem.at[c],
        ).start()

    small = [
        pltpu.make_async_copy(rates_in, rates, small_sem.at[0]),
        pltpu.make_async_copy(shift_in, shift, small_sem.at[1]),
        pltpu.make_async_copy(fraction_in, fraction, small_sem.at[2]),
    ]
    for copy in small:
        copy.start()

    with jax.named_scope("barrier"):
        pl.semaphore_wait(barrier, len(near) + jnp.where(lowers, 1, 0))
    if far:
        pl.semaphore_signal(passed, inc=1, device_id=(near[0], ring), device_id_type=MESH)

    def remote(src, dst, send_sem, recv_sem, device):
        return pltpu.make_async_remote_copy(
            src_ref=src, dst_ref=dst, send_sem=send_sem, recv_sem=recv_sem,
            device_id=device, device_id_type=MESH,
        )

    def out_copy(c, d):
        first, f0, n = chunks[c]
        return remote(
            own.at[pl.ds(f0, n), pl.ds(base(first, d), height(first))],
            gathered[c].at[me], sent.at[0], gather_sem.at[c], (d, ring),
        )

    def back_copy(c, d):
        first, f0, n = chunks[c]
        return remote(
            results[c].at[d],
            landed.at[pl.ds(f0, n), pl.ds(2 + base(first, me), height(first))],
            sent.at[1], home_sem.at[c], (d, ring),
        )

    def bytes_of(ref, semaphore):
        return remote(ref, ref, semaphore, semaphore, (me, ring))

    def arrive(c):
        with jax.named_scope("arrived"):
            bytes_of(gathered[c], gather_sem.at[c]).wait_recv()

    def home(c):
        with jax.named_scope("home"):
            bytes_of(results[c].at[pl.ds(0, group - 1)], home_sem.at[c]).wait_recv()

    def peers():
        return far + near

    def ready(c):
        if c == 0:
            bytes_of(own.at[:, pl.ds(0, group)], in_sem.at[0]).wait_recv()
        if c == 1 and more:
            stages[2].wait()

    for c in range(min(2, count)):
        ready(c)
        for d in near:
            out_copy(c, d).start()
    if far:
        with jax.named_scope("passed"):
            pl.semaphore_wait(passed, 1)
    tell(lowers, told, -1)
    for c in range(count):
        for d in far:
            out_copy(c, d).start()
        if c > 1:
            for d in near:
                out_copy(c, d).start()

    small[0].wait()
    table = rates[...]
    place = lax.broadcasted_iota(jnp.int32, table.shape, 1)
    for j in range(rows + 1):
        column = jnp.sum(
            jnp.where(place == start - 1 + j, table, 0.0), axis=1, keepdims=True
        )
        if j == 0:
            column = jnp.where(ring > 0, column, 0.0)
        if j == rows:
            column = jnp.where(ring < rings - 1, column, 0.0)
        spread = jnp.broadcast_to(column, (polar, width))
        size = jnp.abs(spread)
        rate[j] = spread
        bend[j] = size * (1.0 - size)

    @pl.when(ring == 0)
    def _():
        landed[:, 0:2] = jnp.zeros((nf, 2, polar, width), jnp.float32)

    @pl.when(ring == rings - 1)
    def _():
        landed[:, rows + 2 : rows + 4] = jnp.zeros((nf, 2, polar, width), jnp.float32)

    lane = lax.broadcasted_iota(jnp.int32, (polar, width), 1)
    at_first, at_last = lane == 0, lane == width - 1

    def previous(blocks):
        turned = [pltpu.roll(b, 1, 1) for b in blocks]
        return [jnp.where(at_first, turned[p - 1], turned[p]) for p in range(group)]

    def following(blocks):
        turned = [pltpu.roll(b, width - 1, 1) for b in blocks]
        return [jnp.where(at_last, turned[(p + 1) % group], turned[p]) for p in range(group)]

    cycle = group * width

    def azimuth(c):
        first, f0, n = chunks[c]
        source, target = gathered[c], results[c]
        for k in range(height(first)):
            row = start + base(first, me) + k
            courant = fraction[row]
            ahead = courant > 0.0
            amount = shift[row] + jnp.where(ahead, cycle, cycle - 1)
            whole = lax.rem(amount // width, group)
            part = lax.rem(amount, width)
            size = jnp.abs(courant)
            bent = size * (1.0 - size)
            beyond = lane >= part

            for f in range(n):
                turned = [
                    pltpu.roll(source[lax.rem(p + group - whole, group), f, k], part, 1)
                    for p in range(group)
                ]
                q = [jnp.where(beyond, turned[p], turned[p - 1]) for p in range(group)]
                before = previous(q)
                left = [x - y for x, y in zip(q, before)]
                right = following(left)
                value = [
                    courant * x + bent * half_slope(l, r) for x, l, r in zip(q, left, right)
                ]
                lower = previous(value)
                for p in range(group):
                    kept = jnp.where(ahead, q[p], before[p])
                    target[p, f, k] = kept - (value[p] - lower[p])
        landed[pl.ds(f0, n), pl.ds(2 + base(first, me), height(first))] = target[me]

    ghosts = [
        remote(landed.at[:, pl.ds(2, 2)], landed.at[:, pl.ds(rows + 2, 2)], ghost_send, ghost_recv, (me, jnp.maximum(ring - 1, 0))),
        remote(landed.at[:, pl.ds(rows, 2)], landed.at[:, pl.ds(0, 2)], ghost_send, ghost_recv, (me, jnp.minimum(ring + 1, rings - 1))),
    ]
    inside = jnp.logical_and(below, above)
    ghost_bytes = [
        (inside, bytes_of(landed.at[:, pl.ds(0, 4)], ghost_recv), bytes_of(landed.at[:, pl.ds(0, 4)], ghost_send)),
        (below != above, bytes_of(landed.at[:, pl.ds(0, 2)], ghost_recv), bytes_of(landed.at[:, pl.ds(0, 2)], ghost_send)),
    ]

    def radial(f):
        def cell(i):
            return landed[f, i]

        q1, q2 = cell(1), cell(2)
        d1 = q1 - cell(0)
        d2 = q2 - q1
        h1 = half_slope(d1, d2)
        below = None
        for j in range(rows + 1):
            q3 = cell(j + 3)
            d3 = q3 - q2
            h2 = half_slope(d2, d3)
            c, b = rate[j], bend[j]
            ahead = c > 0.0
            flux = c * jnp.where(ahead, q1, q2) + b * jnp.where(ahead, h1, h2)
            if j > 0:
                out[f, j - 1] = q1 - (flux - below)
            below = flux
            q1, q2, d2, h1 = q2, q3, d3, h2

    edges = 1 if more else count

    small[1].wait()
    small[2].wait()

    @pl.when(lifts)
    def _():
        pl.semaphore_wait(told, 1)

    tell(lifts, from_below, 1)
    for c in range(count):
        arrive(c)
        with jax.named_scope("azimuth"):
            azimuth(c)
        for d in peers():
            back_copy(c, d).start()
        if c == 0:

            @pl.when(lowers)
            def _():
                pl.semaphore_wait(from_below, 1)

            @pl.when(leads)
            def _():
                for d in peers():
                    pl.semaphore_signal(told, inc=1, device_id=(d, ring), device_id_type=MESH)

    @pl.when(jnp.logical_not(leads))
    def _():
        pl.semaphore_wait(told, 1)

    for c in range(edges):
        home(c)

    @pl.when(below)
    def _():
        ghosts[0].start()

    @pl.when(above)
    def _():
        ghosts[1].start()

    for case, received, _ in ghost_bytes:
        pl.when(case)(received.wait_recv)

    for c in range(edges, count):
        first, f0, n = chunks[c]
        home(c)
        with jax.named_scope("radial"):
            for f in range(f0, f0 + n):
                radial(f)
    if not more:
        for f in range(nf):
            radial(f)

    for phase in range(2):
        bytes_of(own.at[:, pl.ds(0, rows - rows // group)], sent.at[phase]).wait_send()
    for case, _, delivered in ghost_bytes:
        pl.when(case)(delivered.wait_send)


def shards(fields, shift, fraction, radial_rate):
    nf, rows, polar, width = fields.shape
    group, rings = lax.axis_size("az"), lax.axis_size("rad")
    chunks = chunks_of(nf, rows, group)
    more = rows // group - 1
    boxes = [
        pltpu.VMEM((group, n, 1 if first else more, polar, width), jnp.float32)
        for first, f0, n in chunks
    ]
    count = len(chunks)
    dma = pltpu.SemaphoreType.DMA
    operands = (fields, shift, fraction, radial_rate.T)
    return pl.pallas_call(
        functools.partial(kernel, group, rings, chunks),
        out_shape=jax.ShapeDtypeStruct(fields.shape, jnp.float32),
        in_specs=[pl.BlockSpec(memory_space=pltpu.HBM)] * 4,
        out_specs=pl.BlockSpec(memory_space=pltpu.VMEM),
        scratch_shapes=[
            pltpu.VMEM((nf, rows, polar, width), jnp.float32),
            pltpu.VMEM((nf, rows + 4, polar, width), jnp.float32),
            pltpu.VMEM((rows + 1, polar, width), jnp.float32),
            pltpu.VMEM((rows + 1, polar, width), jnp.float32),
            pltpu.SMEM(shift.shape, jnp.int32),
            pltpu.SMEM(fraction.shape, jnp.float32),
            pltpu.VMEM(radial_rate.shape[::-1], jnp.float32),
            *boxes,
            *boxes,
            dma((3,)),
            dma((2,)),
            dma((2,)),
            dma((count,)),
            dma((count,)),
            dma,
            dma,
            *[pltpu.SemaphoreType.REGULAR] * 3,
        ],
        compiler_params=pltpu.CompilerParams(
            collective_id=0, has_side_effects=True, vmem_limit_bytes=10 * fields.size * 4
        ),
    )(*(pltpu.with_memory_space_constraint(x, pltpu.HBM) for x in operands))


def solution(mesh):
    placed = (P(None, "rad", None, "az"), P(), P(), P())
    return jax.shard_map(
        shards, mesh=mesh, in_specs=placed, out_specs=P(None, "rad", None, "az"), check_vma=False
    )
```

```python
import functools

import jax
import jax.numpy as jnp
from jax import lax
from jax.experimental import pallas as pl
from jax.experimental.pallas import tpu as pltpu
from jax.sharding import PartitionSpec as P

MESH = pl.DeviceIdType.MESH


def half_slope(left, right):
    low = jnp.maximum(jnp.minimum(left, right), 0.0)
    high = jnp.minimum(jnp.maximum(left, right), 0.0)
    return jnp.maximum(jnp.minimum(0.25 * (left + right), low), high)


def chunks_of(fields, rows, group):
    rest = rows // group - 1
    if rest == 0:
        return [(True, f, 1) for f in range(fields)]
    if lends(rows, group):
        return [(True, 0, fields), (False, 0, fields - 2), (False, fields - 2, 1), (False, fields - 1, 1)]
    return [(True, 0, fields), (False, 0, fields - 2), (False, fields - 2, 2)]


def lends(rows, group):
    return group == 4 and rows > group


def radial(landed, rate, bend, f, target, g):
    rows = rate.shape[0] - 1
    q1, q2 = landed[f, 1], landed[f, 2]
    d1 = q1 - landed[f, 0]
    d2 = q2 - q1
    h1 = half_slope(d1, d2)
    inner = None
    for j in range(rows + 1):
        q3 = landed[f, j + 3]
        d3 = q3 - q2
        h2 = half_slope(d2, d3)
        c, b = rate[j], bend[j]
        ahead = c > 0.0
        flux = c * jnp.where(ahead, q1, q2) + b * jnp.where(ahead, h1, h2)
        if j > 0:
            target[g, j - 1] = q1 - (flux - inner)
        inner = flux
        q1, q2, d2, h1 = q2, q3, d3, h2


def finish(done, landed, rate, bend, out, fresh, sems):
    ready = done.shape[0]
    early = pltpu.make_async_copy(done, out.at[pl.ds(0, ready)], sems.at[0])
    late = pltpu.make_async_copy(fresh, out.at[pl.ds(ready, fresh.shape[0])], sems.at[1])
    early.start()
    for g in range(fresh.shape[0]):
        radial(landed, rate, bend, ready + g, fresh, g)
    late.start()
    early.wait()
    late.wait()


def peers_of(group, me):
    if group == 4:
        inner = me + 1 - 2 * lax.rem(me, 2)
        outer = lax.rem(me + 2, 4)
        return [inner, outer], [inner + outer - me]
    return [lax.rem(me + step, group) for step in range(1, group)], []


def kernel(
    group, rings, chunks,
    fields, shift_in, fraction_in, rates_in,
    out, landed, rate, bend,
    own, shift, fraction, rates, *rest,
):
    count = len(chunks)
    gathered, results = rest[:count], rest[count : 2 * count]
    small_sem, in_sem, sent, gather_sem, home_sem, ghost_send, ghost_recv, passed, told, from_below, *lent = rest[2 * count :]
    lending = lends(fields.shape[1], group)
    if lending:
        lent, lent_sem = lent
        lent_in, lent_out = lent.at[pl.ds(0, group)], lent.at[pl.ds(group, group)]
    nf, rows, polar, width = fields.shape
    me, ring = lax.axis_index("az"), lax.axis_index("rad")
    more = rows // group - 1
    start = ring * rows

    def base(first, d):
        if first:
            return jnp.where(d < 2, d, jnp.where(d < 4, rows - 4 + d, d - 2))
        return group - 2 + d * more

    def height(first):
        return 1 if first else more

    def block(c, d, lift=0):
        first, f0, n = chunks[c]
        return pl.ds(f0, n), pl.ds(lift + base(first, d), height(first))

    near, far = peers_of(group, me)
    barrier = pltpu.get_barrier_semaphore()
    for d in near:
        pl.semaphore_signal(barrier, inc=1, device_id=(d, ring), device_id_type=MESH)

    below, above = ring > 0, ring < rings - 1
    leads = me == 0

    def tell(who, semaphore, step):
        @pl.when(who)
        def _():
            pl.semaphore_signal(semaphore, inc=1, device_id=(me, ring + step), device_id_type=MESH)

    lowers, lifts = jnp.logical_and(leads, below), jnp.logical_and(leads, above)
    tell(lifts, barrier, 1)

    stages = [
        pltpu.make_async_copy(fields.at[:, pl.ds(0, group - 2)], own.at[:, pl.ds(0, group - 2)], in_sem.at[0]),
        pltpu.make_async_copy(fields.at[:, pl.ds(rows - 2, 2)], own.at[:, pl.ds(rows - 2, 2)], in_sem.at[0]),
    ]
    if more:
        stages.append(
            pltpu.make_async_copy(
                fields.at[:, pl.ds(group - 2, rows - group)],
                own.at[:, pl.ds(group - 2, rows - group)],
                in_sem.at[1],
            )
        )
    for copy in stages:
        copy.start()
    lender = ring == 0
    keeps = jnp.logical_or(me != 0, jnp.logical_not(lender))
    helps = jnp.logical_and(me == 3, lender)
    usual = jnp.logical_and(keeps, jnp.logical_not(helps))

    def own_copy(c):
        return pltpu.make_async_copy(fields.at[block(c, me)], gathered[c].at[me], gather_sem.at[c])

    full = count - 1 if lending else count
    for c in range(full):
        own_copy(c).start()
    if lending:
        pl.when(keeps)(own_copy(full).start)

        @pl.when(helps)
        def _():
            pltpu.make_async_copy(fields.at[block(full, 0)], lent_in.at[me], lent_sem).start()

    small = [
        pltpu.make_async_copy(rates_in, rates, small_sem.at[0]),
        pltpu.make_async_copy(shift_in, shift, small_sem.at[1]),
        pltpu.make_async_copy(fraction_in, fraction, small_sem.at[2]),
    ]
    for copy in small:
        copy.start()

    with jax.named_scope("barrier"):
        pl.semaphore_wait(barrier, len(near) + jnp.where(lowers, 1, 0))
    if far:
        pl.semaphore_signal(passed, inc=1, device_id=(near[0], ring), device_id_type=MESH)

    def remote(src, dst, send_sem, recv_sem, device):
        return pltpu.make_async_remote_copy(
            src_ref=src, dst_ref=dst, send_sem=send_sem, recv_sem=recv_sem,
            device_id=device, device_id_type=MESH,
        )

    def out_copy(c, d):
        return remote(
            own.at[block(c, d)], gathered[c].at[me], sent.at[0, c], gather_sem.at[c], (d, ring)
        )

    def back_copy(c, d):
        return remote(
            results[c].at[d], landed.at[block(c, me, 2)], sent.at[1 if c < full else 0, c], home_sem.at[c], (d, ring)
        )

    def lend():
        return remote(own.at[block(full, 0)], lent_in.at[me], sent.at[0, full], lent_sem, (3, ring))

    def give_back(d):
        return remote(lent_out.at[d], landed.at[block(full, 0, 2)], sent.at[0, full], home_sem.at[full], (d, ring))

    def bytes_of(ref, semaphore):
        return remote(ref, ref, semaphore, semaphore, (me, ring))

    def arrive(c):
        with jax.named_scope("arrived"):
            bytes_of(gathered[c], gather_sem.at[c]).wait_recv()

    def home(c):
        with jax.named_scope("home"):
            if c < full:
                bytes_of(results[c].at[pl.ds(0, group - 1)], home_sem.at[c]).wait_recv()
                return
            for who, pieces in ((jnp.logical_not(keeps), 4), (helps, 2), (usual, 3)):
                pl.when(who)(bytes_of(results[c].at[pl.ds(0, pieces)], home_sem.at[c]).wait_recv)

    def peers():
        return far + near

    def ready(c):
        if c == 0:
            bytes_of(own.at[:, pl.ds(0, group)], in_sem.at[0]).wait_recv()
        if c == 1 and more:
            stages[2].wait()

    started = min(2, count)
    for c in range(started):
        ready(c)
        for d in near:
            out_copy(c, d).start()
    if far:
        with jax.named_scope("passed"):
            pl.semaphore_wait(passed, 1)
    tell(lowers, told, -1)
    for c in range(started):
        for d in far:
            out_copy(c, d).start()
    if lending:
        pl.when(jnp.logical_and(lender, me != 3))(lend().start)
    for c in range(started, full):
        for d in near + far:
            out_copy(c, d).start()
    if lending:
        for d in near + far:
            pl.when(jnp.logical_or(d != 0, jnp.logical_not(lender)))(out_copy(full, d).start)

    small[0].wait()
    table = rates[...]
    place = lax.broadcasted_iota(jnp.int32, table.shape, 1)
    for j in range(rows + 1):
        column = jnp.sum(
            jnp.where(place == start - 1 + j, table, 0.0), axis=1, keepdims=True
        )
        if j == 0:
            column = jnp.where(ring > 0, column, 0.0)
        if j == rows:
            column = jnp.where(ring < rings - 1, column, 0.0)
        spread = jnp.broadcast_to(column, (polar, width))
        size = jnp.abs(spread)
        rate[j] = spread
        bend[j] = size * (1.0 - size)

    @pl.when(ring == 0)
    def _():
        landed[:, 0:2] = jnp.zeros((nf, 2, polar, width), jnp.float32)

    @pl.when(ring == rings - 1)
    def _():
        landed[:, rows + 2 : rows + 4] = jnp.zeros((nf, 2, polar, width), jnp.float32)

    lane = lax.broadcasted_iota(jnp.int32, (polar, width), 1)
    at_first, at_last = lane == 0, lane == width - 1

    def previous(blocks):
        turned = [pltpu.roll(b, 1, 1) for b in blocks]
        return [jnp.where(at_first, turned[p - 1], turned[p]) for p in range(group)]

    def following(blocks):
        turned = [pltpu.roll(b, width - 1, 1) for b in blocks]
        return [jnp.where(at_last, turned[(p + 1) % group], turned[p]) for p in range(group)]

    cycle = group * width

    def azimuth(c, source, target, owner):
        first, f0, n = chunks[c]
        for k in range(height(first)):
            row = start + base(first, owner) + k
            courant = fraction[row]
            ahead = courant > 0.0
            amount = shift[row] + jnp.where(ahead, cycle, cycle - 1)
            whole = lax.rem(amount // width, group)
            part = lax.rem(amount, width)
            size = jnp.abs(courant)
            bent = size * (1.0 - size)
            beyond = lane >= part

            for f in range(n):
                turned = [
                    pltpu.roll(source[lax.rem(p + group - whole, group), f, k], part, 1)
                    for p in range(group)
                ]
                q = [jnp.where(beyond, turned[p], turned[p - 1]) for p in range(group)]
                before = previous(q)
                left = [x - y for x, y in zip(q, before)]
                right = following(left)
                value = [
                    courant * x + bent * half_slope(l, r) for x, l, r in zip(q, left, right)
                ]
                lower = previous(value)
                for p in range(group):
                    kept = jnp.where(ahead, q[p], before[p])
                    target[p, f, k] = kept - (value[p] - lower[p])
        landed[block(c, owner, 2)] = target[me]

    ghosts = [
        remote(landed.at[:, pl.ds(2, 2)], landed.at[:, pl.ds(rows + 2, 2)], ghost_send, ghost_recv, (me, jnp.maximum(ring - 1, 0))),
        remote(landed.at[:, pl.ds(rows, 2)], landed.at[:, pl.ds(0, 2)], ghost_send, ghost_recv, (me, jnp.minimum(ring + 1, rings - 1))),
    ]
    inside = jnp.logical_and(below, above)
    ghost_bytes = [
        (inside, bytes_of(landed.at[:, pl.ds(0, 4)], ghost_recv), bytes_of(landed.at[:, pl.ds(0, 4)], ghost_send)),
        (below != above, bytes_of(landed.at[:, pl.ds(0, 2)], ghost_recv), bytes_of(landed.at[:, pl.ds(0, 2)], ghost_send)),
    ]

    edges = 1 if more else count

    small[1].wait()
    small[2].wait()

    @pl.when(lifts)
    def _():
        pl.semaphore_wait(told, 1)

    tell(lifts, from_below, 1)
    for c in range(full):
        arrive(c)
        with jax.named_scope("azimuth"):
            azimuth(c, gathered[c], results[c], me)
        for d in peers():
            if lending and c in (1,) and d is near[0]:
                pl.when(jnp.logical_not(helps))(back_copy(c, d).start)
            else:
                back_copy(c, d).start()
        if lending and c == 1:

            @pl.when(helps)
            def _():
                with jax.named_scope("lent"):
                    bytes_of(lent_in, lent_sem).wait_recv()
                azimuth(full, lent_in, lent_out, 0)
                for d in peers():
                    give_back(d).start()

        if c == 0:

            @pl.when(lowers)
            def _():
                pl.semaphore_wait(from_below, 1)

            @pl.when(leads)
            def _():
                for d in peers():
                    pl.semaphore_signal(told, inc=1, device_id=(d, ring), device_id_type=MESH)

    if lending:

        @pl.when(keeps)
        def _():
            arrive(full)
            azimuth(full, gathered[full], results[full], me)
            for d in peers():
                back_copy(full, d).start()

        @pl.when(helps)
        def _():
            for c in (1,):
                back_copy(c, near[0]).start()

    @pl.when(jnp.logical_not(leads))
    def _():
        pl.semaphore_wait(told, 1)

    for c in range(edges):
        home(c)

    @pl.when(below)
    def _():
        ghosts[0].start()

    @pl.when(above)
    def _():
        ghosts[1].start()

    for case, received, _ in ghost_bytes:
        pl.when(case)(received.wait_recv)

    for c in range(edges, count):
        first, f0, n = chunks[c]
        home(c)
        if f0 < out.shape[0]:
            with jax.named_scope("radial"):
                for f in range(f0, f0 + n):
                    radial(landed, rate, bend, f, out, f)
    if not more:
        for f in range(out.shape[0]):
            radial(landed, rate, bend, f, out, f)

    for c in range(full):
        for phase in range(2):
            bytes_of(results[c].at[pl.ds(0, group - 1)], sent.at[phase, c]).wait_send()
    if lending:
        for who, pieces in ((jnp.logical_not(keeps), 4), (helps, 8), (usual, 6)):
            pl.when(who)(bytes_of(lent.at[pl.ds(0, pieces)], sent.at[0, full]).wait_send)
    for case, _, delivered in ghost_bytes:
        pl.when(case)(delivered.wait_send)


def shards(fields, shift, fraction, radial_rate):
    nf, rows, polar, width = fields.shape
    group, rings = lax.axis_size("az"), lax.axis_size("rad")
    chunks = chunks_of(nf, rows, group)
    more = rows // group - 1
    boxes = [
        pltpu.VMEM((group, n, 1 if first else more, polar, width), jnp.float32)
        for first, f0, n in chunks
    ]
    count = len(chunks)
    dma = pltpu.SemaphoreType.DMA
    lent = []
    if lends(rows, group):
        lent = [pltpu.VMEM((2 * group, 1, more, polar, width), jnp.float32), dma]
    operands = (fields, shift, fraction, radial_rate.T)
    left = chunks[-1][2]

    def like(*shape):
        return jax.ShapeDtypeStruct((*shape, polar, width), jnp.float32)

    vmem, hbm = pl.BlockSpec(memory_space=pltpu.VMEM), pl.BlockSpec(memory_space=pltpu.HBM)
    moved = pl.pallas_call(
        functools.partial(kernel, group, rings, chunks),
        out_shape=[like(nf - left, rows), like(nf, rows + 4), like(rows + 1), like(rows + 1)],
        in_specs=[hbm] * 4,
        out_specs=[vmem] * 4,
        scratch_shapes=[
            pltpu.VMEM((nf, rows, polar, width), jnp.float32),
            pltpu.SMEM(shift.shape, jnp.int32),
            pltpu.SMEM(fraction.shape, jnp.float32),
            pltpu.VMEM(radial_rate.shape[::-1], jnp.float32),
            *boxes,
            *boxes,
            dma((3,)),
            dma((2,)),
            dma((2, count)),
            dma((count,)),
            dma((count,)),
            dma,
            dma,
            *[pltpu.SemaphoreType.REGULAR] * 3,
            *lent,
        ],
        compiler_params=pltpu.CompilerParams(
            collective_id=0, has_side_effects=True, vmem_limit_bytes=10 * fields.size * 4
        ),
    )(*(pltpu.with_memory_space_constraint(x, pltpu.HBM) for x in operands))
    return pl.pallas_call(
        finish,
        out_shape=jax.ShapeDtypeStruct(fields.shape, jnp.float32),
        in_specs=[vmem] * 4,
        out_specs=hbm,
        scratch_shapes=[pltpu.VMEM((left, rows, polar, width), jnp.float32), dma((2,))],
        compiler_params=pltpu.CompilerParams(vmem_limit_bytes=5 * fields.size * 4),
    )(*moved)


def solution(mesh):
    placed = (P(None, "rad", None, "az"), P(), P(), P())
    return jax.shard_map(
        shards, mesh=mesh, in_specs=placed, out_specs=P(None, "rad", None, "az"), check_vma=False
    )
```

```python
import functools

import jax
import jax.numpy as jnp
from jax import lax
from jax.experimental import pallas as pl
from jax.experimental.pallas import tpu as pltpu
from jax.sharding import PartitionSpec as P

MESH = pl.DeviceIdType.MESH


def half_slope(left, right):
    low = jnp.maximum(jnp.minimum(left, right), 0.0)
    high = jnp.minimum(jnp.maximum(left, right), 0.0)
    return jnp.maximum(jnp.minimum(0.25 * (left + right), low), high)


def chunks_of(fields, rows, group):
    rest = rows // group - 1
    if rest == 0:
        return [(True, f, 1) for f in range(fields)]
    if lends(rows, group):
        return [(True, 0, fields), (False, 0, fields - 2), (False, fields - 2, 1), (False, fields - 1, 1)]
    return [(True, 0, fields), (False, 0, fields - 2), (False, fields - 2, 2)]


def lends(rows, group):
    return group == 4 and rows > group


def radial(landed, rate, bend, f, target, g, low, high):
    q1, q2 = landed[f, low + 1], landed[f, low + 2]
    d1 = q1 - landed[f, low]
    d2 = q2 - q1
    h1 = half_slope(d1, d2)
    inner = None
    for j in range(low, high + 1):
        q3 = landed[f, j + 3]
        d3 = q3 - q2
        h2 = half_slope(d2, d3)
        c, b = rate[j], bend[j]
        ahead = c > 0.0
        flux = c * jnp.where(ahead, q1, q2) + b * jnp.where(ahead, h1, h2)
        if j > low:
            target[g, j - 1] = q1 - (flux - inner)
        inner = flux
        q1, q2, d2, h1 = q2, q3, d3, h2


def finish(done, landed, rate, bend, out, fresh, sems):
    ready = done.shape[0]
    early = pltpu.make_async_copy(done, out.at[pl.ds(0, ready)], sems.at[0])
    late = pltpu.make_async_copy(fresh, out.at[pl.ds(ready, fresh.shape[0])], sems.at[1])
    early.start()
    for g in range(fresh.shape[0]):
        radial(landed, rate, bend, ready + g, fresh, g, 0, fresh.shape[1])
    late.start()
    early.wait()
    late.wait()


def peers_of(group, me):
    if group == 4:
        inner = me + 1 - 2 * lax.rem(me, 2)
        outer = lax.rem(me + 2, 4)
        return [inner, outer], [inner + outer - me]
    return [lax.rem(me + step, group) for step in range(1, group)], []


def kernel(
    group, rings, chunks,
    fields, shift_in, fraction_in, rates_in,
    out, landed, rate, bend,
    own, shift, fraction, rates, *rest,
):
    count = len(chunks)
    boxes, rest = rest[:count], rest[count:]
    gathered = [box.at[pl.ds(0, group)] for box in boxes]
    results = [box.at[pl.ds(group, group)] for box in boxes]
    small_sem, in_sem, sent, gather_sem, home_sem, ghost_send, ghost_recv, passed, told, tied, *rest = rest
    lending = lends(fields.shape[1], group)
    if lending:
        lent, lent_sem = rest
        lent_in, lent_out = lent.at[pl.ds(0, group)], lent.at[pl.ds(group, group)]
    nf, rows, polar, width = fields.shape
    me, ring = lax.axis_index("az"), lax.axis_index("rad")
    more = rows // group - 1
    start = ring * rows

    def base(first, d):
        if first:
            return jnp.where(d < 2, d, jnp.where(d < 4, rows - 4 + d, d - 2))
        return group - 2 + d * more

    def height(first):
        return 1 if first else more

    def block(c, d, lift=0):
        first, f0, n = chunks[c]
        return pl.ds(f0, n), pl.ds(lift + base(first, d), height(first))

    near, far = peers_of(group, me)
    stages = [
        pltpu.make_async_copy(fields.at[:, pl.ds(0, group - 2)], own.at[:, pl.ds(0, group - 2)], in_sem.at[0]),
        pltpu.make_async_copy(fields.at[:, pl.ds(rows - 2, 2)], own.at[:, pl.ds(rows - 2, 2)], in_sem.at[0]),
    ]
    if more:
        stages.append(
            pltpu.make_async_copy(
                fields.at[:, pl.ds(group - 2, rows - group)],
                own.at[:, pl.ds(group - 2, rows - group)],
                in_sem.at[1],
            )
        )
    for copy in stages:
        copy.start()

    barrier = pltpu.get_barrier_semaphore()
    between = jnp.logical_or(me == 1, me == 2)

    def greet():
        for d in near:
            pl.semaphore_signal(barrier, inc=1, device_id=(d, ring), device_id_type=MESH)

    if far:
        pl.when(me != 3)(greet)
    else:
        greet()

    below, above = ring > 0, ring < rings - 1
    leads = me == 0

    def tell(who, semaphore, step):
        @pl.when(who)
        def _():
            pl.semaphore_signal(semaphore, inc=1, device_id=(me, ring + step), device_id_type=MESH)

    lowers, lifts = jnp.logical_and(leads, below), jnp.logical_and(leads, above)
    tell(lifts, barrier, 1)

    lender = ring == 0
    keeps = jnp.logical_or(me != 0, jnp.logical_not(lender))
    helps = jnp.logical_and(me == 3, lender)
    usual = jnp.logical_and(keeps, jnp.logical_not(helps))

    def own_copy(c):
        return pltpu.make_async_copy(fields.at[block(c, me)], gathered[c].at[me], gather_sem.at[c])

    full = count - 1 if lending else count
    for c in range(full):
        own_copy(c).start()
    if lending:
        pl.when(keeps)(own_copy(full).start)

        @pl.when(helps)
        def _():
            pltpu.make_async_copy(fields.at[block(full, 0)], lent_in.at[me], lent_sem).start()

    small = [
        pltpu.make_async_copy(rates_in, rates, small_sem.at[0]),
        pltpu.make_async_copy(shift_in, shift, small_sem.at[1]),
        pltpu.make_async_copy(fraction_in, fraction, small_sem.at[2]),
    ]
    for copy in small:
        copy.start()

    with jax.named_scope("barrier"):
        greeted = jnp.where(between, 1, 2) if far else len(near)
        pl.semaphore_wait(barrier, greeted + jnp.where(lowers, 1, 0))
    if far:

        @pl.when(me == 3)
        def _():
            for d in near:
                pl.semaphore_signal(tied, inc=1, device_id=(d, ring), device_id_type=MESH)

    def remote(src, dst, send_sem, recv_sem, device):
        return pltpu.make_async_remote_copy(
            src_ref=src, dst_ref=dst, send_sem=send_sem, recv_sem=recv_sem,
            device_id=device, device_id_type=MESH,
        )

    def out_copy(c, d):
        return remote(own.at[block(c, d)], gathered[c].at[me], sent.at[c], gather_sem.at[c], (d, ring))

    edge_sems = [home_sem.at[i] for i in (0, count, count + 1)] if lending else []

    def back_copy(c, d):
        landing = home_sem.at[c]
        if lending and c == 0:
            landing = edge_sems[[d is other for other in near + far].index(True)]
        return remote(results[c].at[d], landed.at[block(c, me, 2)], sent.at[c], landing, (d, ring))

    def lend():
        return remote(own.at[block(full, 0)], lent_in.at[me], sent.at[full], lent_sem, (3, ring))

    def give_back(d):
        return remote(lent_out.at[d], landed.at[block(full, 0, 2)], sent.at[full], home_sem.at[full], (d, ring))

    def bytes_of(ref, semaphore):
        return remote(ref, ref, semaphore, semaphore, (me, ring))

    def arrive(c):
        with jax.named_scope("arrived"):
            bytes_of(gathered[c], gather_sem.at[c]).wait_recv()

    def home(c):
        with jax.named_scope("home"):
            if c < full:
                bytes_of(results[c].at[pl.ds(0, group - 1)], home_sem.at[c]).wait_recv()
                return
            for who, pieces in ((jnp.logical_not(keeps), 4), (helps, 2), (usual, 3)):
                pl.when(who)(bytes_of(results[c].at[pl.ds(0, pieces)], home_sem.at[c]).wait_recv)

    def peers():
        return far + near

    def ready(c):
        if c == 0:
            bytes_of(own.at[:, pl.ds(0, group)], in_sem.at[0]).wait_recv()
        if c == 1 and more:
            stages[2].wait()

    started = min(2, count)
    if far:
        known = [jnp.logical_or(jnp.logical_not(between), me == k + 1) for k in range(2)]
        for c in range(started):
            with jax.named_scope("ready"):
                ready(c)
            for k in range(2):
                pl.when(known[k])(out_copy(c, near[k]).start)

        @pl.when(between)
        def _():
            with jax.named_scope("answer"):
                pl.semaphore_wait(tied, 1)
            for c in range(started):
                for k in range(2):
                    pl.when(me != k + 1)(out_copy(c, near[k]).start)

        pl.semaphore_signal(passed, inc=1, device_id=(near[0], ring), device_id_type=MESH)
        with jax.named_scope("passed"):
            pl.semaphore_wait(passed, 1)
    else:
        for c in range(started):
            ready(c)
            for d in near:
                out_copy(c, d).start()
    tell(lowers, told, -1)
    for c in range(started):
        for d in far:
            out_copy(c, d).start()
    if lending:
        pl.when(jnp.logical_and(lender, me != 3))(lend().start)
    for c in range(started, full):
        for d in near + far:
            out_copy(c, d).start()
    if lending:
        for d in near + far:
            pl.when(jnp.logical_or(d != 0, jnp.logical_not(lender)))(out_copy(full, d).start)

    small[0].wait()
    table = rates[...]
    place = lax.broadcasted_iota(jnp.int32, table.shape, 1)
    for j in range(rows + 1):
        column = jnp.sum(
            jnp.where(place == start - 1 + j, table, 0.0), axis=1, keepdims=True
        )
        if j == 0:
            column = jnp.where(ring > 0, column, 0.0)
        if j == rows:
            column = jnp.where(ring < rings - 1, column, 0.0)
        spread = jnp.broadcast_to(column, (polar, width))
        size = jnp.abs(spread)
        rate[j] = spread
        bend[j] = size * (1.0 - size)

    @pl.when(ring == 0)
    def _():
        landed[:, 0:2] = jnp.zeros((nf, 2, polar, width), jnp.float32)

    @pl.when(ring == rings - 1)
    def _():
        landed[:, rows + 2 : rows + 4] = jnp.zeros((nf, 2, polar, width), jnp.float32)

    lane = lax.broadcasted_iota(jnp.int32, (polar, width), 1)
    at_first, at_last = lane == 0, lane == width - 1

    def previous(blocks):
        turned = [pltpu.roll(b, 1, 1) for b in blocks]
        return [jnp.where(at_first, turned[p - 1], turned[p]) for p in range(group)]

    def following(blocks):
        turned = [pltpu.roll(b, width - 1, 1) for b in blocks]
        return [jnp.where(at_last, turned[(p + 1) % group], turned[p]) for p in range(group)]

    cycle = group * width

    def azimuth(c, source, target, owner):
        first, f0, n = chunks[c]
        for k in range(height(first)):
            row = start + base(first, owner) + k
            courant = fraction[row]
            ahead = courant > 0.0
            amount = shift[row] + jnp.where(ahead, cycle, cycle - 1)
            whole = lax.rem(amount // width, group)
            part = lax.rem(amount, width)
            size = jnp.abs(courant)
            bent = size * (1.0 - size)
            beyond = lane >= part

            for f in range(n):
                turned = [
                    pltpu.roll(source[lax.rem(p + group - whole, group), f, k], part, 1)
                    for p in range(group)
                ]
                q = [jnp.where(beyond, turned[p], turned[p - 1]) for p in range(group)]
                before = previous(q)
                left = [x - y for x, y in zip(q, before)]
                right = following(left)
                value = [
                    courant * x + bent * half_slope(l, r) for x, l, r in zip(q, left, right)
                ]
                lower = previous(value)
                for p in range(group):
                    kept = jnp.where(ahead, q[p], before[p])
                    target[p, f, k] = kept - (value[p] - lower[p])
        landed[block(c, owner, 2)] = target[me]

    inside = jnp.logical_and(below, above)
    ghost_bytes = [
        (inside, bytes_of(landed.at[:, pl.ds(0, 4)], ghost_recv), bytes_of(landed.at[:, pl.ds(0, 4)], ghost_send)),
        (below != above, bytes_of(landed.at[:, pl.ds(0, 2)], ghost_recv), bytes_of(landed.at[:, pl.ds(0, 2)], ghost_send)),
    ]

    edges = 1 if more else count

    small[1].wait()
    small[2].wait()

    @pl.when(lifts)
    def _():
        pl.semaphore_wait(told, 1)

    tell(lifts, tied, 1)
    for c in range(full):
        arrive(c)
        with jax.named_scope("azimuth"):
            azimuth(c, gathered[c], results[c], me)
        if lending and c == 2:
            for d in (far[0], near[1]):
                pl.when(me == 0)(back_copy(1, d).start)
        for d in peers():
            if lending and c in (1, 2) and d is near[0]:
                pl.when(jnp.logical_not(helps))(back_copy(c, d).start)
            elif lending and c == 1 and d is not near[0]:
                pl.when(me != 0)(back_copy(c, d).start)
            else:
                back_copy(c, d).start()
        if lending and c == 1:

            @pl.when(helps)
            def _():
                with jax.named_scope("lent"):
                    bytes_of(lent_in, lent_sem).wait_recv()
                azimuth(full, lent_in, lent_out, 0)
                for d in (far[0], near[1]):
                    give_back(d).start()

        if c == 0:

            @pl.when(lowers)
            def _():
                pl.semaphore_wait(tied, 1)

            @pl.when(leads)
            def _():
                for d in peers():
                    pl.semaphore_signal(told, inc=1, device_id=(d, ring), device_id_type=MESH)

    if lending:

        @pl.when(keeps)
        def _():
            arrive(full)
            azimuth(full, gathered[full], results[full], me)
            for d in peers():
                if d is near[0]:
                    pl.when(jnp.logical_not(helps))(back_copy(full, d).start)
                else:
                    back_copy(full, d).start()

        @pl.when(helps)
        def _():
            for c in (1, 2):
                back_copy(c, near[0]).start()
            back_copy(full, near[0]).start()
            give_back(near[0]).start()

    @pl.when(jnp.logical_not(leads))
    def _():
        pl.semaphore_wait(told, 1)

    def edge_ghost(d):
        down = d < 2
        row = 2 + base(True, d)
        target = jnp.where(down, rows + 2 + d, d - 2)
        beside = jnp.clip(ring + jnp.where(down, -1, 1), 0, rings - 1)
        copy = remote(
            landed.at[:, pl.ds(row, 1)], landed.at[:, pl.ds(target, 1)], ghost_send, ghost_recv, (me, beside)
        )
        pl.when(jnp.where(down, ring, rings - 1 - ring) > 0)(copy.start)

    if lending:
        edge_ghost(me)
        for k, d in enumerate(near + far):
            with jax.named_scope("edge%d" % k):
                bytes_of(results[0].at[0], edge_sems[k]).wait_recv()
            edge_ghost(d)
    else:
        for c in range(edges):
            home(c)
        for there, row, target, step in ((below, 2, rows + 2, -1), (above, rows, 0, 1)):
            beside = jnp.clip(ring + step, 0, rings - 1)
            copy = remote(
                landed.at[:, pl.ds(row, 2)], landed.at[:, pl.ds(target, 2)], ghost_send, ghost_recv, (me, beside)
            )
            pl.when(there)(copy.start)

    def advance(low_field, fields_in, spans):
        for f in range(low_field, low_field + fields_in):
            for low, high in spans:
                radial(landed, rate, bend, f, out, f, low, high)

    def ghosts_in():
        for case, received, _ in ghost_bytes:
            pl.when(case)(received.wait_recv)

    done = out.shape[0]
    if more and rows > 5:
        _, f0, n = chunks[1]
        home(1)
        advance(f0, n, [(2, rows - 2)])
        ghosts_in()
        advance(f0, n, [(0, 2), (rows - 2, rows)])
        for c in range(2, count):
            _, f0, n = chunks[c]
            home(c)
            if f0 < done:
                advance(f0, n, [(0, rows)])
    else:
        for c in range(edges, count):
            home(c)
        ghosts_in()
        advance(0, done, [(0, rows)])

    for c in range(full):
        bytes_of(boxes[c].at[pl.ds(0, 2 * (group - 1))], sent.at[c]).wait_send()
    if lending:
        for who, pieces in ((jnp.logical_not(keeps), 4), (helps, 8), (usual, 6)):
            pl.when(who)(bytes_of(lent.at[pl.ds(0, pieces)], sent.at[full]).wait_send)
    for case, _, delivered in ghost_bytes:
        pl.when(case)(delivered.wait_send)


def shards(fields, shift, fraction, radial_rate):
    nf, rows, polar, width = fields.shape
    group, rings = lax.axis_size("az"), lax.axis_size("rad")
    chunks = chunks_of(nf, rows, group)
    more = rows // group - 1
    boxes = [
        pltpu.VMEM((2 * group, n, 1 if first else more, polar, width), jnp.float32)
        for first, f0, n in chunks
    ]
    count = len(chunks)
    dma = pltpu.SemaphoreType.DMA
    lent = []
    if lends(rows, group):
        lent = [pltpu.VMEM((2 * group, 1, more, polar, width), jnp.float32), dma]
    operands = (fields, shift, fraction, radial_rate.T)
    left = chunks[-1][2]

    def like(*shape):
        return jax.ShapeDtypeStruct((*shape, polar, width), jnp.float32)

    vmem, hbm = pl.BlockSpec(memory_space=pltpu.VMEM), pl.BlockSpec(memory_space=pltpu.HBM)
    moved = pl.pallas_call(
        functools.partial(kernel, group, rings, chunks),
        out_shape=[like(nf - left, rows), like(nf, rows + 4), like(rows + 1), like(rows + 1)],
        in_specs=[hbm] * 4,
        out_specs=[vmem] * 4,
        scratch_shapes=[
            pltpu.VMEM((nf, rows, polar, width), jnp.float32),
            pltpu.SMEM(shift.shape, jnp.int32),
            pltpu.SMEM(fraction.shape, jnp.float32),
            pltpu.VMEM(radial_rate.shape[::-1], jnp.float32),
            *boxes,
            dma((3,)),
            dma((2,)),
            dma((count,)),
            dma((count,)),
            dma((count + 2 * lends(rows, group),)),
            dma,
            dma,
            *[pltpu.SemaphoreType.REGULAR] * 3,
            *lent,
        ],
        compiler_params=pltpu.CompilerParams(
            collective_id=0, has_side_effects=True, vmem_limit_bytes=10 * fields.size * 4
        ),
    )(*(pltpu.with_memory_space_constraint(x, pltpu.HBM) for x in operands))
    return pl.pallas_call(
        finish,
        out_shape=jax.ShapeDtypeStruct(fields.shape, jnp.float32),
        in_specs=[vmem] * 4,
        out_specs=hbm,
        scratch_shapes=[pltpu.VMEM((left, rows, polar, width), jnp.float32), dma((2,))],
        compiler_params=pltpu.CompilerParams(vmem_limit_bytes=5 * fields.size * 4),
    )(*moved)


def solution(mesh):
    placed = (P(None, "rad", None, "az"), P(), P(), P())
    return jax.shard_map(
        shards, mesh=mesh, in_specs=placed, out_specs=P(None, "rad", None, "az"), check_vma=False
    )
```

```python
import functools

import jax
import jax.numpy as jnp
from jax import lax
from jax.experimental import pallas as pl
from jax.experimental.pallas import tpu as pltpu
from jax.sharding import PartitionSpec as P

MESH = pl.DeviceIdType.MESH


def half_slope(left, right):
    low = jnp.maximum(jnp.minimum(left, right), 0.0)
    high = jnp.minimum(jnp.maximum(left, right), 0.0)
    return jnp.maximum(jnp.minimum(0.25 * (left + right), low), high)


def chunks_of(fields, rows, group):
    rest = rows // group - 1
    if rest == 0:
        return [(True, f, 1) for f in range(fields)]
    if lends(rows, group):
        return [(True, 0, fields), (False, 0, fields - 2), (False, fields - 2, 1), (False, fields - 1, 1)]
    return [(True, 0, fields), (False, 0, fields - 2), (False, fields - 2, 2)]


def lends(rows, group):
    return group == 4 and rows > group


def radial(landed, rate, bend, f, target, g, low, high):
    q1, q2 = landed[f, low + 1], landed[f, low + 2]
    d1 = q1 - landed[f, low]
    d2 = q2 - q1
    h1 = half_slope(d1, d2)
    inner = None
    for j in range(low, high + 1):
        q3 = landed[f, j + 3]
        d3 = q3 - q2
        h2 = half_slope(d2, d3)
        c, b = rate[j], bend[j]
        ahead = c > 0.0
        flux = c * jnp.where(ahead, q1, q2) + b * jnp.where(ahead, h1, h2)
        if j > low:
            target[g, j - 1] = q1 - (flux - inner)
        inner = flux
        q1, q2, d2, h1 = q2, q3, d3, h2


def finish(done, landed, rate, bend, out, fresh, sems):
    ready = done.shape[0]
    early = pltpu.make_async_copy(done, out.at[pl.ds(0, ready)], sems.at[0])
    late = pltpu.make_async_copy(fresh, out.at[pl.ds(ready, fresh.shape[0])], sems.at[1])
    early.start()
    for g in range(fresh.shape[0]):
        radial(landed, rate, bend, ready + g, fresh, g, 0, fresh.shape[1])
    late.start()
    early.wait()
    late.wait()


def peers_of(group, me):
    if group == 4:
        inner = me + 1 - 2 * lax.rem(me, 2)
        outer = lax.rem(me + 2, 4)
        return [inner, outer], [inner + outer - me]
    return [lax.rem(me + step, group) for step in range(1, group)], []


def kernel(
    group, rings, chunks,
    fields, shift_in, fraction_in, rates_in,
    out, landed, rate, bend,
    shift, fraction, rates, *rest,
):
    count = len(chunks)
    boxes, rest = rest[:count], rest[count:]
    gathered = [box.at[pl.ds(0, group)] for box in boxes]
    results = [box.at[pl.ds(group, group)] for box in boxes]
    small_sem, sent, gather_sem, home_sem, ghost_send, ghost_recv, passed, told, tied, *rest = rest
    lending = lends(fields.shape[1], group)
    if lending:
        lent, lent_sem = rest
        lent_in, lent_out = lent.at[pl.ds(0, group)], lent.at[pl.ds(group, group)]
    nf, rows, polar, width = fields.shape
    me, ring = lax.axis_index("az"), lax.axis_index("rad")
    more = rows // group - 1
    start = ring * rows

    def base(first, d):
        if first:
            return jnp.where(d < 2, d, jnp.where(d < 4, rows - 4 + d, d - 2))
        return group - 2 + d * more

    def height(first):
        return 1 if first else more

    def block(c, d, lift=0):
        first, f0, n = chunks[c]
        return pl.ds(f0, n), pl.ds(lift + base(first, d), height(first))

    near, far = peers_of(group, me)
    barrier = pltpu.get_barrier_semaphore()
    between = jnp.logical_or(me == 1, me == 2)

    def greet():
        for d in near:
            pl.semaphore_signal(barrier, inc=1, device_id=(d, ring), device_id_type=MESH)

    if far:
        pl.when(me != 3)(greet)
    else:
        greet()

    below, above = ring > 0, ring < rings - 1
    leads = me == 0

    def tell(who, semaphore, step):
        @pl.when(who)
        def _():
            pl.semaphore_signal(semaphore, inc=1, device_id=(me, ring + step), device_id_type=MESH)

    lowers, lifts = jnp.logical_and(leads, below), jnp.logical_and(leads, above)
    tell(lifts, barrier, 1)

    lender = ring == 0
    keeps = jnp.logical_or(me != 0, jnp.logical_not(lender))
    helps = jnp.logical_and(me == 3, lender)
    usual = jnp.logical_and(keeps, jnp.logical_not(helps))

    def own_copy(c):
        return pltpu.make_async_copy(fields.at[block(c, me)], gathered[c].at[me], gather_sem.at[c])

    full = count - 1 if lending else count
    for c in range(full):
        own_copy(c).start()
    if lending:
        pl.when(keeps)(own_copy(full).start)

        @pl.when(helps)
        def _():
            pltpu.make_async_copy(fields.at[block(full, 0)], lent_in.at[me], lent_sem).start()

    small = [
        pltpu.make_async_copy(rates_in, rates, small_sem.at[0]),
        pltpu.make_async_copy(shift_in, shift, small_sem.at[1]),
        pltpu.make_async_copy(fraction_in, fraction, small_sem.at[2]),
    ]
    for copy in small:
        copy.start()

    with jax.named_scope("barrier"):
        greeted = jnp.where(between, 1, 2) if far else len(near)
        pl.semaphore_wait(barrier, greeted + jnp.where(lowers, 1, 0))
    if far:

        @pl.when(me == 3)
        def _():
            for d in near:
                pl.semaphore_signal(tied, inc=1, device_id=(d, ring), device_id_type=MESH)

    def remote(src, dst, send_sem, recv_sem, device):
        return pltpu.make_async_remote_copy(
            src_ref=src, dst_ref=dst, send_sem=send_sem, recv_sem=recv_sem,
            device_id=device, device_id_type=MESH,
        )

    def out_copy(c, d):
        return remote(fields.at[block(c, d)], gathered[c].at[me], sent.at[c], gather_sem.at[c], (d, ring))

    edge_sems = [home_sem.at[i] for i in (0, count, count + 1)] if lending else []

    def back_copy(c, d):
        landing = home_sem.at[c]
        if lending and c == 0:
            landing = edge_sems[[d is other for other in near + far].index(True)]
        return remote(results[c].at[d], landed.at[block(c, me, 2)], sent.at[c], landing, (d, ring))

    def lend():
        return remote(fields.at[block(full, 0)], lent_in.at[me], sent.at[full], lent_sem, (3, ring))

    def give_back(d):
        return remote(lent_out.at[d], landed.at[block(full, 0, 2)], sent.at[full], home_sem.at[full], (d, ring))

    def bytes_of(ref, semaphore):
        return remote(ref, ref, semaphore, semaphore, (me, ring))

    def arrive(c):
        with jax.named_scope("arrived"):
            bytes_of(gathered[c], gather_sem.at[c]).wait_recv()

    def home(c):
        with jax.named_scope("home"):
            if c < full:
                bytes_of(results[c].at[pl.ds(0, group - 1)], home_sem.at[c]).wait_recv()
                return
            for who, pieces in ((jnp.logical_not(keeps), 4), (helps, 2), (usual, 3)):
                pl.when(who)(bytes_of(results[c].at[pl.ds(0, pieces)], home_sem.at[c]).wait_recv)

    def peers():
        return far + near

    started = min(2, count)
    if far:
        known = [jnp.logical_or(jnp.logical_not(between), me == k + 1) for k in range(2)]
        for c in range(started):
            for k in range(2):
                pl.when(known[k])(out_copy(c, near[k]).start)

        @pl.when(between)
        def _():
            with jax.named_scope("answer"):
                pl.semaphore_wait(tied, 1)
            for c in range(started):
                for k in range(2):
                    pl.when(me != k + 1)(out_copy(c, near[k]).start)

        pl.semaphore_signal(passed, inc=1, device_id=(near[0], ring), device_id_type=MESH)
        with jax.named_scope("passed"):
            pl.semaphore_wait(passed, 1)
    else:
        for c in range(started):
            for d in near:
                out_copy(c, d).start()
    tell(lowers, told, -1)
    for c in range(started):
        for d in far:
            out_copy(c, d).start()
    if lending:
        pl.when(jnp.logical_and(lender, me != 3))(lend().start)
    for c in range(started, full):
        for d in near + far:
            out_copy(c, d).start()
    if lending:
        for d in near + far:
            pl.when(jnp.logical_or(d != 0, jnp.logical_not(lender)))(out_copy(full, d).start)

    small[0].wait()
    table = rates[...]
    place = lax.broadcasted_iota(jnp.int32, table.shape, 1)
    for j in range(rows + 1):
        column = jnp.sum(
            jnp.where(place == start - 1 + j, table, 0.0), axis=1, keepdims=True
        )
        if j == 0:
            column = jnp.where(ring > 0, column, 0.0)
        if j == rows:
            column = jnp.where(ring < rings - 1, column, 0.0)
        spread = jnp.broadcast_to(column, (polar, width))
        size = jnp.abs(spread)
        rate[j] = spread
        bend[j] = size * (1.0 - size)

    @pl.when(ring == 0)
    def _():
        landed[:, 0:2] = jnp.zeros((nf, 2, polar, width), jnp.float32)

    @pl.when(ring == rings - 1)
    def _():
        landed[:, rows + 2 : rows + 4] = jnp.zeros((nf, 2, polar, width), jnp.float32)

    lane = lax.broadcasted_iota(jnp.int32, (polar, width), 1)
    at_first, at_last = lane == 0, lane == width - 1

    def previous(blocks):
        turned = [pltpu.roll(b, 1, 1) for b in blocks]
        return [jnp.where(at_first, turned[p - 1], turned[p]) for p in range(group)]

    def following(blocks):
        turned = [pltpu.roll(b, width - 1, 1) for b in blocks]
        return [jnp.where(at_last, turned[(p + 1) % group], turned[p]) for p in range(group)]

    cycle = group * width

    def azimuth(c, source, target, owner):
        first, f0, n = chunks[c]
        for k in range(height(first)):
            row = start + base(first, owner) + k
            courant = fraction[row]
            ahead = courant > 0.0
            amount = shift[row] + jnp.where(ahead, cycle, cycle - 1)
            whole = lax.rem(amount // width, group)
            part = lax.rem(amount, width)
            size = jnp.abs(courant)
            bent = size * (1.0 - size)
            beyond = lane >= part

            for f in range(n):
                turned = [
                    pltpu.roll(source[lax.rem(p + group - whole, group), f, k], part, 1)
                    for p in range(group)
                ]
                q = [jnp.where(beyond, turned[p], turned[p - 1]) for p in range(group)]
                before = previous(q)
                left = [x - y for x, y in zip(q, before)]
                right = following(left)
                value = [
                    courant * x + bent * half_slope(l, r) for x, l, r in zip(q, left, right)
                ]
                lower = previous(value)
                for p in range(group):
                    kept = jnp.where(ahead, q[p], before[p])
                    target[p, f, k] = kept - (value[p] - lower[p])
        landed[block(c, owner, 2)] = target[me]

    inside = jnp.logical_and(below, above)
    ghost_bytes = [
        (inside, bytes_of(landed.at[:, pl.ds(0, 4)], ghost_recv), bytes_of(landed.at[:, pl.ds(0, 4)], ghost_send)),
        (below != above, bytes_of(landed.at[:, pl.ds(0, 2)], ghost_recv), bytes_of(landed.at[:, pl.ds(0, 2)], ghost_send)),
    ]

    edges = 1 if more else count

    small[1].wait()
    small[2].wait()

    @pl.when(lifts)
    def _():
        pl.semaphore_wait(told, 1)

    tell(lifts, tied, 1)
    for c in range(full):
        arrive(c)
        with jax.named_scope("azimuth"):
            azimuth(c, gathered[c], results[c], me)
        if lending and c == 2:
            for d in (far[0], near[1]):
                pl.when(me == 0)(back_copy(1, d).start)
        for d in peers():
            if lending and c in (1, 2) and d is near[0]:
                pl.when(jnp.logical_not(helps))(back_copy(c, d).start)
            elif lending and c == 1 and d is not near[0]:
                pl.when(me != 0)(back_copy(c, d).start)
            else:
                back_copy(c, d).start()
        if lending and c == 1:

            @pl.when(helps)
            def _():
                with jax.named_scope("lent"):
                    bytes_of(lent_in, lent_sem).wait_recv()
                azimuth(full, lent_in, lent_out, 0)
                for d in (far[0], near[1]):
                    give_back(d).start()

        if c == 0:

            @pl.when(lowers)
            def _():
                pl.semaphore_wait(tied, 1)

            @pl.when(leads)
            def _():
                for d in peers():
                    pl.semaphore_signal(told, inc=1, device_id=(d, ring), device_id_type=MESH)

    if lending:

        @pl.when(keeps)
        def _():
            arrive(full)
            azimuth(full, gathered[full], results[full], me)
            for d in peers():
                if d is near[0]:
                    pl.when(jnp.logical_not(helps))(back_copy(full, d).start)
                else:
                    back_copy(full, d).start()

        @pl.when(helps)
        def _():
            for c in (1, 2):
                back_copy(c, near[0]).start()
            back_copy(full, near[0]).start()
            give_back(near[0]).start()

    @pl.when(jnp.logical_not(leads))
    def _():
        pl.semaphore_wait(told, 1)

    def edge_ghost(d):
        down = d < 2
        row = 2 + base(True, d)
        target = jnp.where(down, rows + 2 + d, d - 2)
        beside = jnp.clip(ring + jnp.where(down, -1, 1), 0, rings - 1)
        copy = remote(
            landed.at[:, pl.ds(row, 1)], landed.at[:, pl.ds(target, 1)], ghost_send, ghost_recv, (me, beside)
        )
        pl.when(jnp.where(down, ring, rings - 1 - ring) > 0)(copy.start)

    if lending:
        edge_ghost(me)
        for k, d in enumerate(near + far):
            with jax.named_scope("edge%d" % k):
                bytes_of(results[0].at[0], edge_sems[k]).wait_recv()
            edge_ghost(d)
    else:
        for c in range(edges):
            home(c)
        for there, row, target, step in ((below, 2, rows + 2, -1), (above, rows, 0, 1)):
            beside = jnp.clip(ring + step, 0, rings - 1)
            copy = remote(
                landed.at[:, pl.ds(row, 2)], landed.at[:, pl.ds(target, 2)], ghost_send, ghost_recv, (me, beside)
            )
            pl.when(there)(copy.start)

    def advance(low_field, fields_in, spans):
        for f in range(low_field, low_field + fields_in):
            for low, high in spans:
                radial(landed, rate, bend, f, out, f, low, high)

    def ghosts_in():
        for case, received, _ in ghost_bytes:
            pl.when(case)(received.wait_recv)

    done = out.shape[0]
    if more and rows > 5:
        _, f0, n = chunks[1]
        home(1)
        advance(f0, n, [(2, rows - 2)])
        ghosts_in()
        advance(f0, n, [(0, 2), (rows - 2, rows)])
        for c in range(2, count):
            _, f0, n = chunks[c]
            home(c)
            if f0 < done:
                advance(f0, n, [(0, rows)])
    else:
        for c in range(edges, count):
            home(c)
        ghosts_in()
        advance(0, done, [(0, rows)])

    for c in range(full):
        bytes_of(boxes[c].at[pl.ds(0, 2 * (group - 1))], sent.at[c]).wait_send()
    if lending:
        for who, pieces in ((jnp.logical_not(keeps), 4), (helps, 8), (usual, 6)):
            pl.when(who)(bytes_of(lent.at[pl.ds(0, pieces)], sent.at[full]).wait_send)
    for case, _, delivered in ghost_bytes:
        pl.when(case)(delivered.wait_send)


def shards(fields, shift, fraction, radial_rate):
    nf, rows, polar, width = fields.shape
    group, rings = lax.axis_size("az"), lax.axis_size("rad")
    chunks = chunks_of(nf, rows, group)
    more = rows // group - 1
    boxes = [
        pltpu.VMEM((2 * group, n, 1 if first else more, polar, width), jnp.float32)
        for first, f0, n in chunks
    ]
    count = len(chunks)
    dma = pltpu.SemaphoreType.DMA
    lent = []
    if lends(rows, group):
        lent = [pltpu.VMEM((2 * group, 1, more, polar, width), jnp.float32), dma]
    operands = (fields, shift, fraction, radial_rate.T)
    left = chunks[-1][2]

    def like(*shape):
        return jax.ShapeDtypeStruct((*shape, polar, width), jnp.float32)

    vmem, hbm = pl.BlockSpec(memory_space=pltpu.VMEM), pl.BlockSpec(memory_space=pltpu.HBM)
    moved = pl.pallas_call(
        functools.partial(kernel, group, rings, chunks),
        out_shape=[like(nf - left, rows), like(nf, rows + 4), like(rows + 1), like(rows + 1)],
        in_specs=[hbm] * 4,
        out_specs=[vmem] * 4,
        scratch_shapes=[
            pltpu.SMEM(shift.shape, jnp.int32),
            pltpu.SMEM(fraction.shape, jnp.float32),
            pltpu.VMEM(radial_rate.shape[::-1], jnp.float32),
            *boxes,
            dma((3,)),
            dma((count,)),
            dma((count,)),
            dma((count + 2 * lends(rows, group),)),
            dma,
            dma,
            *[pltpu.SemaphoreType.REGULAR] * 3,
            *lent,
        ],
        compiler_params=pltpu.CompilerParams(
            collective_id=0, has_side_effects=True, vmem_limit_bytes=10 * fields.size * 4
        ),
    )(*(pltpu.with_memory_space_constraint(x, pltpu.HBM) for x in operands))
    return pl.pallas_call(
        finish,
        out_shape=jax.ShapeDtypeStruct(fields.shape, jnp.float32),
        in_specs=[vmem] * 4,
        out_specs=hbm,
        scratch_shapes=[pltpu.VMEM((left, rows, polar, width), jnp.float32), dma((2,))],
        compiler_params=pltpu.CompilerParams(vmem_limit_bytes=5 * fields.size * 4),
    )(*moved)


def solution(mesh):
    placed = (P(None, "rad", None, "az"), P(), P(), P())
    return jax.shard_map(
        shards, mesh=mesh, in_specs=placed, out_specs=P(None, "rad", None, "az"), check_vma=False
    )
```

```python
import functools

import jax
import jax.numpy as jnp
from jax import lax
from jax.experimental import pallas as pl
from jax.experimental.pallas import tpu as pltpu
from jax.sharding import PartitionSpec as P

MESH = pl.DeviceIdType.MESH


def half_slope(left, right):
    low = jnp.maximum(jnp.minimum(left, right), 0.0)
    high = jnp.minimum(jnp.maximum(left, right), 0.0)
    return jnp.maximum(jnp.minimum(0.25 * (left + right), low), high)


def chunks_of(fields, rows, group):
    rest = rows // group - 1
    if rest == 0:
        return [(True, f, 1) for f in range(fields)]
    if lends(rows, group):
        return [(True, 0, fields), (False, 0, fields - 2), (False, fields - 2, 1), (False, fields - 1, 1)]
    return [(True, 0, fields), (False, 0, fields - 2), (False, fields - 2, 2)]


def lends(rows, group):
    return group == 4 and rows > group


def radial(landed, rate, bend, f, target, g, low, high):
    q1, q2 = landed[f, low + 1], landed[f, low + 2]
    d1 = q1 - landed[f, low]
    d2 = q2 - q1
    h1 = half_slope(d1, d2)
    inner = None
    for j in range(low, high + 1):
        q3 = landed[f, j + 3]
        d3 = q3 - q2
        h2 = half_slope(d2, d3)
        c, b = rate[j], bend[j]
        ahead = c > 0.0
        flux = c * jnp.where(ahead, q1, q2) + b * jnp.where(ahead, h1, h2)
        if j > low:
            target[g, j - 1] = q1 - (flux - inner)
        inner = flux
        q1, q2, d2, h1 = q2, q3, d3, h2


def finish(done, landed, rate, bend, out, fresh, sems):
    ready = done.shape[0]
    early = pltpu.make_async_copy(done, out.at[pl.ds(0, ready)], sems.at[0])
    late = pltpu.make_async_copy(fresh, out.at[pl.ds(ready, fresh.shape[0])], sems.at[1])
    early.start()
    for g in range(fresh.shape[0]):
        radial(landed, rate, bend, ready + g, fresh, g, 0, fresh.shape[1])
    late.start()
    early.wait()
    late.wait()


def peers_of(group, me):
    if group == 4:
        inner = me + 1 - 2 * lax.rem(me, 2)
        outer = lax.rem(me + 2, 4)
        return [inner, outer], [inner + outer - me]
    return [lax.rem(me + step, group) for step in range(1, group)], []


def kernel(
    group, rings, chunks,
    fields, shift_in, fraction_in, rates_in,
    out, landed, rate, bend,
    shift, fraction, rates, *rest,
):
    count = len(chunks)
    boxes, rest = rest[:count], rest[count:]
    gathered = [box.at[pl.ds(0, group)] for box in boxes]
    results = [box.at[pl.ds(group, group)] for box in boxes]
    small_sem, sent, gather_sem, home_sem, ghost_send, ghost_recv, passed, told, tied, *rest = rest
    lending = lends(fields.shape[1], group)
    if lending:
        lent, lent_sem = rest
        lent_in, lent_out = lent.at[pl.ds(0, group)], lent.at[pl.ds(group, group)]
    nf, rows, polar, width = fields.shape
    me, ring = lax.axis_index("az"), lax.axis_index("rad")
    more = rows // group - 1
    start = ring * rows

    def base(first, d):
        if first:
            return jnp.where(d < 2, d, jnp.where(d < 4, rows - 4 + d, d - 2))
        return group - 2 + d * more

    def height(first):
        return 1 if first else more

    def block(c, d, lift=0):
        first, f0, n = chunks[c]
        return pl.ds(f0, n), pl.ds(lift + base(first, d), height(first))

    near, far = peers_of(group, me)
    barrier = pltpu.get_barrier_semaphore()
    between = jnp.logical_or(me == 1, me == 2)

    def greet():
        for d in near:
            pl.semaphore_signal(barrier, inc=1, device_id=(d, ring), device_id_type=MESH)

    if far:
        pl.when(me != 3)(greet)
    else:
        greet()

    below, above = ring > 0, ring < rings - 1
    leads = me == 0

    def tell(who, semaphore, step):
        @pl.when(who)
        def _():
            pl.semaphore_signal(semaphore, inc=1, device_id=(me, ring + step), device_id_type=MESH)

    lowers, lifts = jnp.logical_and(leads, below), jnp.logical_and(leads, above)
    tell(lifts, barrier, 1)

    lender = ring == 0
    keeps = jnp.logical_or(me != 0, jnp.logical_not(lender))
    helps = jnp.logical_and(me == 3, lender)
    usual = jnp.logical_and(keeps, jnp.logical_not(helps))

    def own_copy(c):
        return pltpu.make_async_copy(fields.at[block(c, me)], gathered[c].at[me], gather_sem.at[c])

    full = count - 1 if lending else count
    for c in range(full):
        own_copy(c).start()
    if lending:
        pl.when(keeps)(own_copy(full).start)

        @pl.when(helps)
        def _():
            pltpu.make_async_copy(fields.at[block(full, 0)], lent_in.at[me], lent_sem).start()

    small = [
        pltpu.make_async_copy(rates_in, rates, small_sem.at[0]),
        pltpu.make_async_copy(shift_in, shift, small_sem.at[1]),
        pltpu.make_async_copy(fraction_in, fraction, small_sem.at[2]),
    ]
    for copy in small:
        copy.start()

    with jax.named_scope("barrier"):
        greeted = jnp.where(between, 1, 2) if far else len(near)
        pl.semaphore_wait(barrier, greeted + jnp.where(lowers, 1, 0))
    if far:

        @pl.when(me == 3)
        def _():
            for d in near:
                pl.semaphore_signal(tied, inc=1, device_id=(d, ring), device_id_type=MESH)

    def remote(src, dst, send_sem, recv_sem, device):
        return pltpu.make_async_remote_copy(
            src_ref=src, dst_ref=dst, send_sem=send_sem, recv_sem=recv_sem,
            device_id=device, device_id_type=MESH,
        )

    def out_copy(c, d):
        return remote(fields.at[block(c, d)], gathered[c].at[me], sent.at[c], gather_sem.at[c], (d, ring))

    edge_sems = [home_sem.at[i] for i in (0, count, count + 1)] if lending else []

    def back_copy(c, d):
        landing = home_sem.at[c]
        if lending and c == 0:
            landing = edge_sems[[d is other for other in near + far].index(True)]
        return remote(results[c].at[d], landed.at[block(c, me, 2)], sent.at[c], landing, (d, ring))

    def lend():
        return remote(fields.at[block(full, 0)], lent_in.at[me], sent.at[full], lent_sem, (3, ring))

    def give_back(d):
        return remote(lent_out.at[d], landed.at[block(full, 0, 2)], sent.at[full], home_sem.at[full], (d, ring))

    def bytes_of(ref, semaphore):
        return remote(ref, ref, semaphore, semaphore, (me, ring))

    def arrive(c):
        with jax.named_scope("arrived"):
            bytes_of(gathered[c], gather_sem.at[c]).wait_recv()

    def home(c):
        with jax.named_scope("home"):
            if c < full:
                bytes_of(results[c].at[pl.ds(0, group - 1)], home_sem.at[c]).wait_recv()
                return
            for who, pieces in ((jnp.logical_not(keeps), 4), (helps, 2), (usual, 3)):
                pl.when(who)(bytes_of(results[c].at[pl.ds(0, pieces)], home_sem.at[c]).wait_recv)

    def peers():
        return far + near

    if far:
        known = [jnp.logical_or(jnp.logical_not(between), me == k + 1) for k in range(2)]
        for k in range(2):
            pl.when(known[k])(out_copy(0, near[k]).start)

        @pl.when(between)
        def _():
            with jax.named_scope("answer"):
                pl.semaphore_wait(tied, 1)
            for k in range(2):
                pl.when(me != k + 1)(out_copy(0, near[k]).start)

        pl.semaphore_signal(passed, inc=1, device_id=(near[0], ring), device_id_type=MESH)
        with jax.named_scope("passed"):
            pl.semaphore_wait(passed, 1)
    else:
        for d in near:
            out_copy(0, d).start()
    tell(lowers, told, -1)
    for c in range(full):
        for d in far + near if c else far:
            out_copy(c, d).start()
        if lending and c == 1:
            pl.when(jnp.logical_and(lender, me != 3))(lend().start)
    if lending:
        for d in far + near:
            pl.when(jnp.logical_or(d != 0, jnp.logical_not(lender)))(out_copy(full, d).start)

    small[0].wait()
    table = rates[...]
    place = lax.broadcasted_iota(jnp.int32, table.shape, 1)
    for j in range(rows + 1):
        column = jnp.sum(
            jnp.where(place == start - 1 + j, table, 0.0), axis=1, keepdims=True
        )
        if j == 0:
            column = jnp.where(ring > 0, column, 0.0)
        if j == rows:
            column = jnp.where(ring < rings - 1, column, 0.0)
        spread = jnp.broadcast_to(column, (polar, width))
        size = jnp.abs(spread)
        rate[j] = spread
        bend[j] = size * (1.0 - size)

    @pl.when(ring == 0)
    def _():
        landed[:, 0:2] = jnp.zeros((nf, 2, polar, width), jnp.float32)

    @pl.when(ring == rings - 1)
    def _():
        landed[:, rows + 2 : rows + 4] = jnp.zeros((nf, 2, polar, width), jnp.float32)

    lane = lax.broadcasted_iota(jnp.int32, (polar, width), 1)
    at_first, at_last = lane == 0, lane == width - 1

    def previous(blocks):
        turned = [pltpu.roll(b, 1, 1) for b in blocks]
        return [jnp.where(at_first, turned[p - 1], turned[p]) for p in range(group)]

    def following(blocks):
        turned = [pltpu.roll(b, width - 1, 1) for b in blocks]
        return [jnp.where(at_last, turned[(p + 1) % group], turned[p]) for p in range(group)]

    cycle = group * width

    def azimuth(c, source, target, owner):
        first, f0, n = chunks[c]
        for k in range(height(first)):
            row = start + base(first, owner) + k
            courant = fraction[row]
            ahead = courant > 0.0
            amount = shift[row] + jnp.where(ahead, cycle, cycle - 1)
            whole = lax.rem(amount // width, group)
            part = lax.rem(amount, width)
            size = jnp.abs(courant)
            bent = size * (1.0 - size)
            beyond = lane >= part

            for f in range(n):
                turned = [
                    pltpu.roll(source[lax.rem(p + group - whole, group), f, k], part, 1)
                    for p in range(group)
                ]
                q = [jnp.where(beyond, turned[p], turned[p - 1]) for p in range(group)]
                before = previous(q)
                left = [x - y for x, y in zip(q, before)]
                right = following(left)
                value = [
                    courant * x + bent * half_slope(l, r) for x, l, r in zip(q, left, right)
                ]
                lower = previous(value)
                for p in range(group):
                    kept = jnp.where(ahead, q[p], before[p])
                    target[p, f, k] = kept - (value[p] - lower[p])
        landed[block(c, owner, 2)] = target[me]

    inside = jnp.logical_and(below, above)
    ghost_bytes = [
        (inside, bytes_of(landed.at[:, pl.ds(0, 4)], ghost_recv), bytes_of(landed.at[:, pl.ds(0, 4)], ghost_send)),
        (below != above, bytes_of(landed.at[:, pl.ds(0, 2)], ghost_recv), bytes_of(landed.at[:, pl.ds(0, 2)], ghost_send)),
    ]

    edges = 1 if more else count

    small[1].wait()
    small[2].wait()

    @pl.when(lifts)
    def _():
        pl.semaphore_wait(told, 1)

    tell(lifts, tied, 1)
    for c in range(full):
        arrive(c)
        with jax.named_scope("azimuth"):
            azimuth(c, gathered[c], results[c], me)
        if lending and c == 2:
            pl.when(me < 2)(back_copy(1, far[0]).start)
            pl.when(me == 0)(back_copy(1, near[1]).start)
        for d in peers():
            if lending and c in (1, 2) and d is near[0]:
                pl.when(jnp.logical_not(helps))(back_copy(c, d).start)
            elif lending and c == 1 and d is not near[0]:
                pl.when(me > 1 if d is far[0] else me != 0)(back_copy(c, d).start)
            else:
                back_copy(c, d).start()
        if lending and c == 1:

            @pl.when(helps)
            def _():
                with jax.named_scope("lent"):
                    bytes_of(lent_in, lent_sem).wait_recv()
                azimuth(full, lent_in, lent_out, 0)
                for d in (far[0], near[1]):
                    give_back(d).start()

        if c == 0:

            @pl.when(lowers)
            def _():
                pl.semaphore_wait(tied, 1)

            @pl.when(leads)
            def _():
                for d in peers():
                    pl.semaphore_signal(told, inc=1, device_id=(d, ring), device_id_type=MESH)

    if lending:

        @pl.when(keeps)
        def _():
            arrive(full)
            azimuth(full, gathered[full], results[full], me)
            for d in peers():
                if d is near[0]:
                    pl.when(jnp.logical_not(helps))(back_copy(full, d).start)
                else:
                    back_copy(full, d).start()

        @pl.when(helps)
        def _():
            for c in (1, 2):
                back_copy(c, near[0]).start()
            back_copy(full, near[0]).start()
            give_back(near[0]).start()

    @pl.when(jnp.logical_not(leads))
    def _():
        pl.semaphore_wait(told, 1)

    def edge_ghost(d):
        down = d < 2
        row = 2 + base(True, d)
        target = jnp.where(down, rows + 2 + d, d - 2)
        beside = jnp.clip(ring + jnp.where(down, -1, 1), 0, rings - 1)
        copy = remote(
            landed.at[:, pl.ds(row, 1)], landed.at[:, pl.ds(target, 1)], ghost_send, ghost_recv, (me, beside)
        )
        pl.when(jnp.where(down, ring, rings - 1 - ring) > 0)(copy.start)

    if lending:
        edge_ghost(me)
        for k, d in enumerate(near + far):
            with jax.named_scope("edge%d" % k):
                bytes_of(results[0].at[0], edge_sems[k]).wait_recv()
            edge_ghost(d)
    else:
        for c in range(edges):
            home(c)
        for there, row, target, step in ((below, 2, rows + 2, -1), (above, rows, 0, 1)):
            beside = jnp.clip(ring + step, 0, rings - 1)
            copy = remote(
                landed.at[:, pl.ds(row, 2)], landed.at[:, pl.ds(target, 2)], ghost_send, ghost_recv, (me, beside)
            )
            pl.when(there)(copy.start)

    def advance(low_field, fields_in, spans):
        for f in range(low_field, low_field + fields_in):
            for low, high in spans:
                radial(landed, rate, bend, f, out, f, low, high)

    def ghosts_in():
        for case, received, _ in ghost_bytes:
            pl.when(case)(received.wait_recv)

    done = out.shape[0]
    if more and rows > 5:
        _, f0, n = chunks[1]
        home(1)
        advance(f0, n, [(2, rows - 2)])
        ghosts_in()
        advance(f0, n, [(0, 2), (rows - 2, rows)])
        for c in range(2, count):
            _, f0, n = chunks[c]
            home(c)
            if f0 < done:
                advance(f0, n, [(0, rows)])
    else:
        for c in range(edges, count):
            home(c)
        ghosts_in()
        advance(0, done, [(0, rows)])

    for c in range(full):
        bytes_of(boxes[c].at[pl.ds(0, 2 * (group - 1))], sent.at[c]).wait_send()
    if lending:
        for who, pieces in ((jnp.logical_not(keeps), 4), (helps, 8), (usual, 6)):
            pl.when(who)(bytes_of(lent.at[pl.ds(0, pieces)], sent.at[full]).wait_send)
    for case, _, delivered in ghost_bytes:
        pl.when(case)(delivered.wait_send)


def shards(fields, shift, fraction, radial_rate):
    nf, rows, polar, width = fields.shape
    group, rings = lax.axis_size("az"), lax.axis_size("rad")
    chunks = chunks_of(nf, rows, group)
    more = rows // group - 1
    boxes = [
        pltpu.VMEM((2 * group, n, 1 if first else more, polar, width), jnp.float32)
        for first, f0, n in chunks
    ]
    count = len(chunks)
    dma = pltpu.SemaphoreType.DMA
    lent = []
    if lends(rows, group):
        lent = [pltpu.VMEM((2 * group, 1, more, polar, width), jnp.float32), dma]
    operands = (fields, shift, fraction, radial_rate.T)
    left = chunks[-1][2]

    def like(*shape):
        return jax.ShapeDtypeStruct((*shape, polar, width), jnp.float32)

    vmem, hbm = pl.BlockSpec(memory_space=pltpu.VMEM), pl.BlockSpec(memory_space=pltpu.HBM)
    moved = pl.pallas_call(
        functools.partial(kernel, group, rings, chunks),
        out_shape=[like(nf - left, rows), like(nf, rows + 4), like(rows + 1), like(rows + 1)],
        in_specs=[hbm] * 4,
        out_specs=[vmem] * 4,
        scratch_shapes=[
            pltpu.SMEM(shift.shape, jnp.int32),
            pltpu.SMEM(fraction.shape, jnp.float32),
            pltpu.VMEM(radial_rate.shape[::-1], jnp.float32),
            *boxes,
            dma((3,)),
            dma((count,)),
            dma((count,)),
            dma((count + 2 * lends(rows, group),)),
            dma,
            dma,
            *[pltpu.SemaphoreType.REGULAR] * 3,
            *lent,
        ],
        compiler_params=pltpu.CompilerParams(
            collective_id=0, has_side_effects=True, vmem_limit_bytes=10 * fields.size * 4
        ),
    )(*(pltpu.with_memory_space_constraint(x, pltpu.HBM) for x in operands))
    return pl.pallas_call(
        finish,
        out_shape=jax.ShapeDtypeStruct(fields.shape, jnp.float32),
        in_specs=[vmem] * 4,
        out_specs=hbm,
        scratch_shapes=[pltpu.VMEM((left, rows, polar, width), jnp.float32), dma((2,))],
        compiler_params=pltpu.CompilerParams(vmem_limit_bytes=5 * fields.size * 4),
    )(*moved)


def solution(mesh):
    placed = (P(None, "rad", None, "az"), P(), P(), P())
    return jax.shard_map(
        shards, mesh=mesh, in_specs=placed, out_specs=P(None, "rad", None, "az"), check_vma=False
    )
```

```python
import functools

import jax
import jax.numpy as jnp
from jax import lax
from jax.experimental import pallas as pl
from jax.experimental.pallas import tpu as pltpu
from jax.sharding import PartitionSpec as P

MESH = pl.DeviceIdType.MESH


def half_slope(left, right):
    low = jnp.maximum(jnp.minimum(left, right), 0.0)
    high = jnp.minimum(jnp.maximum(left, right), 0.0)
    return jnp.maximum(jnp.minimum(0.25 * (left + right), low), high)


def chunks_of(fields, rows, group):
    rest = rows // group - 1
    if rest == 0:
        return [(True, f, 1) for f in range(fields)]
    if lends(rows, group):
        return [(True, 0, fields), (False, 0, fields - 2), (False, fields - 2, 1), (False, fields - 1, 1)]
    return [(True, 0, fields), (False, 0, fields - 2), (False, fields - 2, 2)]


def lends(rows, group):
    return group == 4 and rows > group


def radial(landed, rate, bend, f, target, g, low, high):
    q1, q2 = landed[f, low + 1], landed[f, low + 2]
    d1 = q1 - landed[f, low]
    d2 = q2 - q1
    h1 = half_slope(d1, d2)
    inner = None
    for j in range(low, high + 1):
        q3 = landed[f, j + 3]
        d3 = q3 - q2
        h2 = half_slope(d2, d3)
        c, b = rate[j], bend[j]
        ahead = c > 0.0
        flux = c * jnp.where(ahead, q1, q2) + b * jnp.where(ahead, h1, h2)
        if j > low:
            target[g, j - 1] = q1 - (flux - inner)
        inner = flux
        q1, q2, d2, h1 = q2, q3, d3, h2


def finish(done, landed, rate, bend, out, fresh, sems):
    ready = done.shape[0]
    early = pltpu.make_async_copy(done, out.at[pl.ds(0, ready)], sems.at[0])
    late = pltpu.make_async_copy(fresh, out.at[pl.ds(ready, fresh.shape[0])], sems.at[1])
    early.start()
    for g in range(fresh.shape[0]):
        radial(landed, rate, bend, ready + g, fresh, g, 0, fresh.shape[1])
    late.start()
    early.wait()
    late.wait()


def peers_of(group, me):
    if group == 4:
        inner = me + 1 - 2 * lax.rem(me, 2)
        outer = lax.rem(me + 2, 4)
        return [inner, outer], [inner + outer - me]
    return [lax.rem(me + step, group) for step in range(1, group)], []


def kernel(
    group, rings, chunks,
    fields, shift_in, fraction_in, rates_in,
    out, landed, rate, bend,
    shift, fraction, rates, *rest,
):
    count = len(chunks)
    boxes, rest = rest[:count], rest[count:]
    gathered = [box.at[pl.ds(0, group)] for box in boxes]
    results = [box.at[pl.ds(group, group)] for box in boxes]
    small_sem, sent, gather_sem, home_sem, ghost_send, ghost_recv, passed, told, tied, *rest = rest
    lending = lends(fields.shape[1], group)
    if lending:
        lent, lent_sem = rest
        lent_in, lent_out = lent.at[pl.ds(0, group)], lent.at[pl.ds(group, group)]
    nf, rows, polar, width = fields.shape
    me, ring = lax.axis_index("az"), lax.axis_index("rad")
    more = rows // group - 1
    start = ring * rows

    def base(first, d):
        if first:
            return jnp.where(d < 2, d, jnp.where(d < 4, rows - 4 + d, d - 2))
        return group - 2 + d * more

    def height(first):
        return 1 if first else more

    def block(c, d, lift=0):
        first, f0, n = chunks[c]
        return pl.ds(f0, n), pl.ds(lift + base(first, d), height(first))

    near, far = peers_of(group, me)
    barrier = pltpu.get_barrier_semaphore()
    between = jnp.logical_or(me == 1, me == 2)

    def greet():
        for d in near:
            pl.semaphore_signal(barrier, inc=1, device_id=(d, ring), device_id_type=MESH)

    if far:
        pl.when(me != 3)(greet)
    else:
        greet()

    below, above = ring > 0, ring < rings - 1
    leads = me == 0

    def tell(who, semaphore, step):
        @pl.when(who)
        def _():
            pl.semaphore_signal(semaphore, inc=1, device_id=(me, ring + step), device_id_type=MESH)

    lowers, lifts = jnp.logical_and(leads, below), jnp.logical_and(leads, above)
    tell(lifts, barrier, 1)

    lender = ring == 0
    keeps = jnp.logical_or(me != 0, jnp.logical_not(lender))
    helps = jnp.logical_and(me == 3, lender)
    usual = jnp.logical_and(keeps, jnp.logical_not(helps))
    defers = jnp.logical_and(me > 1, lax.rem(ring, 2) == 0)

    def own_copy(c):
        return pltpu.make_async_copy(fields.at[block(c, me)], gathered[c].at[me], gather_sem.at[c])

    full = count - 1 if lending else count
    for c in range(full):
        own_copy(c).start()
    if lending:
        pl.when(keeps)(own_copy(full).start)

        @pl.when(helps)
        def _():
            pltpu.make_async_copy(fields.at[block(full, 0)], lent_in.at[me], lent_sem).start()

    small = [
        pltpu.make_async_copy(rates_in, rates, small_sem.at[0]),
        pltpu.make_async_copy(shift_in, shift, small_sem.at[1]),
        pltpu.make_async_copy(fraction_in, fraction, small_sem.at[2]),
    ]
    for copy in small:
        copy.start()

    with jax.named_scope("barrier"):
        greeted = jnp.where(between, 1, 2) if far else len(near)
        pl.semaphore_wait(barrier, greeted + jnp.where(lowers, 1, 0))
    if far:

        @pl.when(me == 3)
        def _():
            for d in near:
                pl.semaphore_signal(tied, inc=1, device_id=(d, ring), device_id_type=MESH)

    def remote(src, dst, send_sem, recv_sem, device):
        return pltpu.make_async_remote_copy(
            src_ref=src, dst_ref=dst, send_sem=send_sem, recv_sem=recv_sem,
            device_id=device, device_id_type=MESH,
        )

    def out_copy(c, d):
        return remote(fields.at[block(c, d)], gathered[c].at[me], sent.at[c], gather_sem.at[c], (d, ring))

    edge_sems = [home_sem.at[i] for i in (0, count, count + 1)] if lending else []

    def back_copy(c, d):
        landing = home_sem.at[c]
        if lending and c == 0:
            landing = edge_sems[[d is other for other in near + far].index(True)]
        return remote(results[c].at[d], landed.at[block(c, me, 2)], sent.at[c], landing, (d, ring))

    def lend():
        return remote(fields.at[block(full, 0)], lent_in.at[me], sent.at[full], lent_sem, (3, ring))

    def give_back(d):
        return remote(lent_out.at[d], landed.at[block(full, 0, 2)], sent.at[full], home_sem.at[full], (d, ring))

    def bytes_of(ref, semaphore):
        return remote(ref, ref, semaphore, semaphore, (me, ring))

    def arrive(c):
        with jax.named_scope("arrived"):
            bytes_of(gathered[c], gather_sem.at[c]).wait_recv()

    def home(c):
        with jax.named_scope("home"):
            if c < full:
                bytes_of(results[c].at[pl.ds(0, group - 1)], home_sem.at[c]).wait_recv()
                return
            for who, pieces in ((jnp.logical_not(keeps), 4), (helps, 2), (usual, 3)):
                pl.when(who)(bytes_of(results[c].at[pl.ds(0, pieces)], home_sem.at[c]).wait_recv)

    def peers():
        return far + near

    if far:
        known = [jnp.logical_or(jnp.logical_not(between), me == k + 1) for k in range(2)]
        for k in range(2):
            pl.when(known[k])(out_copy(0, near[k]).start)

        @pl.when(between)
        def _():
            with jax.named_scope("answer"):
                pl.semaphore_wait(tied, 1)
            for k in range(2):
                pl.when(me != k + 1)(out_copy(0, near[k]).start)

        pl.semaphore_signal(passed, inc=1, device_id=(near[0], ring), device_id_type=MESH)
        with jax.named_scope("passed"):
            pl.semaphore_wait(passed, 1)
    else:
        for d in near:
            out_copy(0, d).start()
    tell(lowers, told, -1)
    for c in range(full):
        for d in far + near if c else far:
            out_copy(c, d).start()
        if lending and c == 1:
            pl.when(jnp.logical_and(lender, me != 3))(lend().start)
    if lending:
        for d in far + near:
            pl.when(jnp.logical_or(d != 0, jnp.logical_not(lender)))(out_copy(full, d).start)

    small[0].wait()
    table = rates[...]
    place = lax.broadcasted_iota(jnp.int32, table.shape, 1)
    for j in range(rows + 1):
        column = jnp.sum(
            jnp.where(place == start - 1 + j, table, 0.0), axis=1, keepdims=True
        )
        if j == 0:
            column = jnp.where(ring > 0, column, 0.0)
        if j == rows:
            column = jnp.where(ring < rings - 1, column, 0.0)
        spread = jnp.broadcast_to(column, (polar, width))
        size = jnp.abs(spread)
        rate[j] = spread
        bend[j] = size * (1.0 - size)

    @pl.when(ring == 0)
    def _():
        landed[:, 0:2] = jnp.zeros((nf, 2, polar, width), jnp.float32)

    @pl.when(ring == rings - 1)
    def _():
        landed[:, rows + 2 : rows + 4] = jnp.zeros((nf, 2, polar, width), jnp.float32)

    lane = lax.broadcasted_iota(jnp.int32, (polar, width), 1)
    at_first, at_last = lane == 0, lane == width - 1

    def previous(blocks):
        turned = [pltpu.roll(b, 1, 1) for b in blocks]
        return [jnp.where(at_first, turned[p - 1], turned[p]) for p in range(group)]

    def following(blocks):
        turned = [pltpu.roll(b, width - 1, 1) for b in blocks]
        return [jnp.where(at_last, turned[(p + 1) % group], turned[p]) for p in range(group)]

    cycle = group * width

    def azimuth(c, source, target, owner):
        first, f0, n = chunks[c]
        for k in range(height(first)):
            row = start + base(first, owner) + k
            courant = fraction[row]
            ahead = courant > 0.0
            amount = shift[row] + jnp.where(ahead, cycle, cycle - 1)
            whole = lax.rem(amount // width, group)
            part = lax.rem(amount, width)
            size = jnp.abs(courant)
            bent = size * (1.0 - size)
            beyond = lane >= part

            for f in range(n):
                turned = [
                    pltpu.roll(source[lax.rem(p + group - whole, group), f, k], part, 1)
                    for p in range(group)
                ]
                q = [jnp.where(beyond, turned[p], turned[p - 1]) for p in range(group)]
                before = previous(q)
                left = [x - y for x, y in zip(q, before)]
                right = following(left)
                value = [
                    courant * x + bent * half_slope(l, r) for x, l, r in zip(q, left, right)
                ]
                lower = previous(value)
                for p in range(group):
                    kept = jnp.where(ahead, q[p], before[p])
                    target[p, f, k] = kept - (value[p] - lower[p])
        landed[block(c, owner, 2)] = target[me]

    inside = jnp.logical_and(below, above)
    ghost_bytes = [
        (inside, bytes_of(landed.at[:, pl.ds(0, 4)], ghost_recv), bytes_of(landed.at[:, pl.ds(0, 4)], ghost_send)),
        (below != above, bytes_of(landed.at[:, pl.ds(0, 2)], ghost_recv), bytes_of(landed.at[:, pl.ds(0, 2)], ghost_send)),
    ]

    edges = 1 if more else count

    small[1].wait()
    small[2].wait()

    @pl.when(lifts)
    def _():
        pl.semaphore_wait(told, 1)

    tell(lifts, tied, 1)
    for c in range(full):
        arrive(c)
        with jax.named_scope("azimuth"):
            azimuth(c, gathered[c], results[c], me)
        if lending and c == 2:
            pl.when(me < 2)(back_copy(1, far[0]).start)
            pl.when(me == 0)(back_copy(1, near[1]).start)
        for d in peers():
            if lending and c in (1, 2) and d is near[0]:
                pl.when(jnp.logical_not(defers))(back_copy(c, d).start)
            elif lending and c == 1 and d is not near[0]:
                pl.when(me > 1 if d is far[0] else me != 0)(back_copy(c, d).start)
            else:
                back_copy(c, d).start()
        if lending and c == 1:

            @pl.when(helps)
            def _():
                with jax.named_scope("lent"):
                    bytes_of(lent_in, lent_sem).wait_recv()
                azimuth(full, lent_in, lent_out, 0)
                for d in (far[0], near[1]):
                    give_back(d).start()

        if c == 0:

            @pl.when(lowers)
            def _():
                pl.semaphore_wait(tied, 1)

            @pl.when(leads)
            def _():
                for d in peers():
                    pl.semaphore_signal(told, inc=1, device_id=(d, ring), device_id_type=MESH)

    if lending:

        @pl.when(keeps)
        def _():
            arrive(full)
            azimuth(full, gathered[full], results[full], me)
            for d in peers():
                if d is near[0]:
                    pl.when(jnp.logical_not(defers))(back_copy(full, d).start)
                else:
                    back_copy(full, d).start()

        @pl.when(defers)
        def _():
            for c in (*(1, 2), full):
                back_copy(c, near[0]).start()

        pl.when(helps)(give_back(near[0]).start)

    @pl.when(jnp.logical_not(leads))
    def _():
        pl.semaphore_wait(told, 1)

    def edge_ghost(d):
        down = d < 2
        row = 2 + base(True, d)
        target = jnp.where(down, rows + 2 + d, d - 2)
        beside = jnp.clip(ring + jnp.where(down, -1, 1), 0, rings - 1)
        copy = remote(
            landed.at[:, pl.ds(row, 1)], landed.at[:, pl.ds(target, 1)], ghost_send, ghost_recv, (me, beside)
        )
        pl.when(jnp.where(down, ring, rings - 1 - ring) > 0)(copy.start)

    if lending:
        edge_ghost(me)
        for k, d in enumerate(near + far):
            with jax.named_scope("edge%d" % k):
                bytes_of(results[0].at[0], edge_sems[k]).wait_recv()
            edge_ghost(d)
    else:
        for c in range(edges):
            home(c)
        for there, row, target, step in ((below, 2, rows + 2, -1), (above, rows, 0, 1)):
            beside = jnp.clip(ring + step, 0, rings - 1)
            copy = remote(
                landed.at[:, pl.ds(row, 2)], landed.at[:, pl.ds(target, 2)], ghost_send, ghost_recv, (me, beside)
            )
            pl.when(there)(copy.start)

    def advance(low_field, fields_in, spans):
        for f in range(low_field, low_field + fields_in):
            for low, high in spans:
                radial(landed, rate, bend, f, out, f, low, high)

    def ghosts_in():
        for case, received, _ in ghost_bytes:
            pl.when(case)(received.wait_recv)

    done = out.shape[0]
    if more and rows > 5:
        _, f0, n = chunks[1]
        home(1)
        advance(f0, n, [(2, rows - 2)])
        ghosts_in()
        advance(f0, n, [(0, 2), (rows - 2, rows)])
        for c in range(2, count):
            _, f0, n = chunks[c]
            home(c)
            if f0 < done:
                advance(f0, n, [(0, rows)])
    else:
        for c in range(edges, count):
            home(c)
        ghosts_in()
        advance(0, done, [(0, rows)])

    for c in range(full):
        bytes_of(boxes[c].at[pl.ds(0, 2 * (group - 1))], sent.at[c]).wait_send()
    if lending:
        for who, pieces in ((jnp.logical_not(keeps), 4), (helps, 8), (usual, 6)):
            pl.when(who)(bytes_of(lent.at[pl.ds(0, pieces)], sent.at[full]).wait_send)
    for case, _, delivered in ghost_bytes:
        pl.when(case)(delivered.wait_send)


def shards(fields, shift, fraction, radial_rate):
    nf, rows, polar, width = fields.shape
    group, rings = lax.axis_size("az"), lax.axis_size("rad")
    chunks = chunks_of(nf, rows, group)
    more = rows // group - 1
    boxes = [
        pltpu.VMEM((2 * group, n, 1 if first else more, polar, width), jnp.float32)
        for first, f0, n in chunks
    ]
    count = len(chunks)
    dma = pltpu.SemaphoreType.DMA
    lent = []
    if lends(rows, group):
        lent = [pltpu.VMEM((2 * group, 1, more, polar, width), jnp.float32), dma]
    operands = (fields, shift, fraction, radial_rate.T)
    left = chunks[-1][2]

    def like(*shape):
        return jax.ShapeDtypeStruct((*shape, polar, width), jnp.float32)

    vmem, hbm = pl.BlockSpec(memory_space=pltpu.VMEM), pl.BlockSpec(memory_space=pltpu.HBM)
    moved = pl.pallas_call(
        functools.partial(kernel, group, rings, chunks),
        out_shape=[like(nf - left, rows), like(nf, rows + 4), like(rows + 1), like(rows + 1)],
        in_specs=[hbm] * 4,
        out_specs=[vmem] * 4,
        scratch_shapes=[
            pltpu.SMEM(shift.shape, jnp.int32),
            pltpu.SMEM(fraction.shape, jnp.float32),
            pltpu.VMEM(radial_rate.shape[::-1], jnp.float32),
            *boxes,
            dma((3,)),
            dma((count,)),
            dma((count,)),
            dma((count + 2 * lends(rows, group),)),
            dma,
            dma,
            *[pltpu.SemaphoreType.REGULAR] * 3,
            *lent,
        ],
        compiler_params=pltpu.CompilerParams(
            collective_id=0, has_side_effects=True, vmem_limit_bytes=10 * fields.size * 4
        ),
    )(*(pltpu.with_memory_space_constraint(x, pltpu.HBM) for x in operands))
    return pl.pallas_call(
        finish,
        out_shape=jax.ShapeDtypeStruct(fields.shape, jnp.float32),
        in_specs=[vmem] * 4,
        out_specs=hbm,
        scratch_shapes=[pltpu.VMEM((left, rows, polar, width), jnp.float32), dma((2,))],
        compiler_params=pltpu.CompilerParams(vmem_limit_bytes=5 * fields.size * 4),
    )(*moved)


def solution(mesh):
    placed = (P(None, "rad", None, "az"), P(), P(), P())
    return jax.shard_map(
        shards, mesh=mesh, in_specs=placed, out_specs=P(None, "rad", None, "az"), check_vma=False
    )
```

```python
import functools

import jax
import jax.numpy as jnp
from jax import lax
from jax.experimental import pallas as pl
from jax.experimental.pallas import tpu as pltpu
from jax.sharding import PartitionSpec as P

MESH = pl.DeviceIdType.MESH


def half_slope(left, right):
    low = jnp.maximum(jnp.minimum(left, right), 0.0)
    high = jnp.minimum(jnp.maximum(left, right), 0.0)
    return jnp.maximum(jnp.minimum(0.25 * (left + right), low), high)


def chunks_of(fields, rows, group):
    rest = rows // group - 1
    if rest == 0:
        return [(True, f, 1) for f in range(fields)]
    if lends(rows, group):
        return [(True, 0, fields), (False, 0, fields - 2), (False, fields - 2, 1), (False, fields - 1, 1)]
    return [(True, 0, fields), (False, 0, fields - 2), (False, fields - 2, 2)]


def lends(rows, group):
    return group == 4 and rows > group


def radial(landed, rate, bend, f, target, g, low, high):
    q1, q2 = landed[f, low + 1], landed[f, low + 2]
    d1 = q1 - landed[f, low]
    d2 = q2 - q1
    h1 = half_slope(d1, d2)
    inner = None
    for j in range(low, high + 1):
        q3 = landed[f, j + 3]
        d3 = q3 - q2
        h2 = half_slope(d2, d3)
        c, b = rate[j], bend[j]
        ahead = c > 0.0
        flux = c * jnp.where(ahead, q1, q2) + b * jnp.where(ahead, h1, h2)
        if j > low:
            target[g, j - 1] = q1 - (flux - inner)
        inner = flux
        q1, q2, d2, h1 = q2, q3, d3, h2


def finish(done, landed, rate, bend, out, fresh, sems):
    ready = done.shape[0]
    early = pltpu.make_async_copy(done, out.at[pl.ds(0, ready)], sems.at[0])
    late = pltpu.make_async_copy(fresh, out.at[pl.ds(ready, fresh.shape[0])], sems.at[1])
    early.start()
    for g in range(fresh.shape[0]):
        radial(landed, rate, bend, ready + g, fresh, g, 0, fresh.shape[1])
    late.start()
    early.wait()
    late.wait()


def peers_of(group, me):
    if group == 4:
        inner = me + 1 - 2 * lax.rem(me, 2)
        outer = lax.rem(me + 2, 4)
        return [inner, outer], [inner + outer - me]
    return [lax.rem(me + step, group) for step in range(1, group)], []


def kernel(
    group, rings, chunks,
    fields, shift_in, fraction_in, rates_in,
    out, landed, rate, bend,
    shift, fraction, rates, *rest,
):
    count = len(chunks)
    boxes, rest = rest[:count], rest[count:]
    gathered = [box.at[pl.ds(0, group)] for box in boxes]
    results = [box.at[pl.ds(group, group)] for box in boxes]
    small_sem, sent, gather_sem, home_sem, ghost_send, ghost_recv, passed, told, tied, *rest = rest
    lending = lends(fields.shape[1], group)
    if lending:
        lent, lent_sem = rest
        lent_in, lent_out = lent.at[pl.ds(0, group)], lent.at[pl.ds(group, group)]
    nf, rows, polar, width = fields.shape
    me, ring = lax.axis_index("az"), lax.axis_index("rad")
    more = rows // group - 1
    start = ring * rows

    def base(first, d):
        if first:
            return jnp.where(d < 2, d, jnp.where(d < 4, rows - 4 + d, d - 2))
        return group - 2 + d * more

    def height(first):
        return 1 if first else more

    def block(c, d, lift=0):
        first, f0, n = chunks[c]
        return pl.ds(f0, n), pl.ds(lift + base(first, d), height(first))

    near, far = peers_of(group, me)
    barrier = pltpu.get_barrier_semaphore()
    between = jnp.logical_or(me == 1, me == 2)

    def greet():
        for d in near:
            pl.semaphore_signal(barrier, inc=1, device_id=(d, ring), device_id_type=MESH)

    if far:
        pl.when(me != 3)(greet)
    else:
        greet()

    below, above = ring > 0, ring < rings - 1
    leads = me == 0

    def tell(who, semaphore, step):
        @pl.when(who)
        def _():
            pl.semaphore_signal(semaphore, inc=1, device_id=(me, ring + step), device_id_type=MESH)

    lowers, lifts = jnp.logical_and(leads, below), jnp.logical_and(leads, above)
    tell(lifts, barrier, 1)

    lender = ring == 0
    keeps = jnp.logical_or(me != 0, jnp.logical_not(lender))
    helps = jnp.logical_and(me == 3, lender)
    usual = jnp.logical_and(keeps, jnp.logical_not(helps))
    defers = jnp.logical_and(me > 1, lax.rem(ring, 2) == 0)

    def own_copy(c):
        return pltpu.make_async_copy(fields.at[block(c, me)], gathered[c].at[me], gather_sem.at[c])

    full = count - 1 if lending else count
    for c in range(full):
        own_copy(c).start()
    if lending:
        pl.when(keeps)(own_copy(full).start)

        @pl.when(helps)
        def _():
            pltpu.make_async_copy(fields.at[block(full, 0)], lent_in.at[me], lent_sem).start()

    small = [
        pltpu.make_async_copy(rates_in, rates, small_sem.at[0]),
        pltpu.make_async_copy(shift_in, shift, small_sem.at[1]),
        pltpu.make_async_copy(fraction_in, fraction, small_sem.at[2]),
    ]
    for copy in small:
        copy.start()

    with jax.named_scope("barrier"):
        greeted = jnp.where(between, 1, 2) if far else len(near)
        pl.semaphore_wait(barrier, greeted + jnp.where(lowers, 1, 0))
    if far:

        @pl.when(me == 3)
        def _():
            for d in near:
                pl.semaphore_signal(tied, inc=1, device_id=(d, ring), device_id_type=MESH)

    def remote(src, dst, send_sem, recv_sem, device):
        return pltpu.make_async_remote_copy(
            src_ref=src, dst_ref=dst, send_sem=send_sem, recv_sem=recv_sem,
            device_id=device, device_id_type=MESH,
        )

    def out_copy(c, d):
        return remote(fields.at[block(c, d)], gathered[c].at[me], sent.at[c], gather_sem.at[c], (d, ring))

    edge_sems = [home_sem.at[i] for i in (0, count, count + 1)] if lending else []

    def back_copy(c, d):
        landing = home_sem.at[c]
        if lending and c == 0:
            landing = edge_sems[[d is other for other in near + far].index(True)]
        return remote(results[c].at[d], landed.at[block(c, me, 2)], sent.at[c], landing, (d, ring))

    def lend():
        return remote(fields.at[block(full, 0)], lent_in.at[me], sent.at[full], lent_sem, (3, ring))

    def give_back(d):
        return remote(lent_out.at[d], landed.at[block(full, 0, 2)], sent.at[full], home_sem.at[full], (d, ring))

    def bytes_of(ref, semaphore):
        return remote(ref, ref, semaphore, semaphore, (me, ring))

    def arrive(c):
        with jax.named_scope("arrived"):
            bytes_of(gathered[c], gather_sem.at[c]).wait_recv()

    def home(c):
        with jax.named_scope("home"):
            if c < full:
                bytes_of(results[c].at[pl.ds(0, group - 1)], home_sem.at[c]).wait_recv()
                return
            for who, pieces in ((jnp.logical_not(keeps), 4), (helps, 2), (usual, 3)):
                pl.when(who)(bytes_of(results[c].at[pl.ds(0, pieces)], home_sem.at[c]).wait_recv)

    def peers():
        return far + near

    if far:
        known = [jnp.logical_or(jnp.logical_not(between), me == k + 1) for k in range(2)]
        for k in range(2):
            pl.when(known[k])(out_copy(0, near[k]).start)

        @pl.when(between)
        def _():
            with jax.named_scope("answer"):
                pl.semaphore_wait(tied, 1)
            for k in range(2):
                pl.when(me != k + 1)(out_copy(0, near[k]).start)

        pl.semaphore_signal(passed, inc=1, device_id=(near[0], ring), device_id_type=MESH)
        with jax.named_scope("passed"):
            pl.semaphore_wait(passed, 1)
    else:
        for d in near:
            out_copy(0, d).start()
    tell(lowers, told, -1)
    for c in range(full):
        for d in far + near if c else far:
            out_copy(c, d).start()
        if lending and c == 1:
            pl.when(jnp.logical_and(lender, me != 3))(lend().start)
    if lending:
        for d in far + near:
            pl.when(jnp.logical_or(d != 0, jnp.logical_not(lender)))(out_copy(full, d).start)

    small[0].wait()
    table = rates[...]
    place = lax.broadcasted_iota(jnp.int32, table.shape, 1)
    for j in range(rows + 1):
        column = jnp.sum(
            jnp.where(place == start - 1 + j, table, 0.0), axis=1, keepdims=True
        )
        if j == 0:
            column = jnp.where(ring > 0, column, 0.0)
        if j == rows:
            column = jnp.where(ring < rings - 1, column, 0.0)
        spread = jnp.broadcast_to(column, (polar, width))
        size = jnp.abs(spread)
        rate[j] = spread
        bend[j] = size * (1.0 - size)

    @pl.when(ring == 0)
    def _():
        landed[:, 0:2] = jnp.zeros((nf, 2, polar, width), jnp.float32)

    @pl.when(ring == rings - 1)
    def _():
        landed[:, rows + 2 : rows + 4] = jnp.zeros((nf, 2, polar, width), jnp.float32)

    lane = lax.broadcasted_iota(jnp.int32, (polar, width), 1)
    at_first, at_last = lane == 0, lane == width - 1

    def previous(blocks):
        turned = [pltpu.roll(b, 1, 1) for b in blocks]
        return [jnp.where(at_first, turned[p - 1], turned[p]) for p in range(group)]

    def following(blocks):
        turned = [pltpu.roll(b, width - 1, 1) for b in blocks]
        return [jnp.where(at_last, turned[(p + 1) % group], turned[p]) for p in range(group)]

    cycle = group * width

    def azimuth(c, source, target, owner):
        first, f0, n = chunks[c]
        for k in range(height(first)):
            row = start + base(first, owner) + k
            courant = fraction[row]
            ahead = courant > 0.0
            amount = shift[row] + jnp.where(ahead, cycle, cycle - 1)
            whole = lax.rem(amount // width, group)
            part = lax.rem(amount, width)
            size = jnp.abs(courant)
            bent = size * (1.0 - size)
            beyond = lane >= part

            for f in range(n):
                turned = [
                    pltpu.roll(source[lax.rem(p + group - whole, group), f, k], part, 1)
                    for p in range(group)
                ]
                q = [jnp.where(beyond, turned[p], turned[p - 1]) for p in range(group)]
                before = previous(q)
                left = [x - y for x, y in zip(q, before)]
                right = following(left)
                value = [
                    courant * x + bent * half_slope(l, r) for x, l, r in zip(q, left, right)
                ]
                lower = previous(value)
                for p in range(group):
                    kept = jnp.where(ahead, q[p], before[p])
                    target[p, f, k] = kept - (value[p] - lower[p])
        landed[block(c, owner, 2)] = target[me]

    inside = jnp.logical_and(below, above)
    ghost_bytes = [
        (inside, bytes_of(landed.at[:, pl.ds(0, 4)], ghost_recv), bytes_of(landed.at[:, pl.ds(0, 4)], ghost_send)),
        (below != above, bytes_of(landed.at[:, pl.ds(0, 2)], ghost_recv), bytes_of(landed.at[:, pl.ds(0, 2)], ghost_send)),
    ]

    edges = 1 if more else count

    small[1].wait()
    small[2].wait()

    @pl.when(lifts)
    def _():
        pl.semaphore_wait(told, 1)

    tell(lifts, tied, 1)
    for c in range(full):
        arrive(c)
        with jax.named_scope("azimuth"):
            azimuth(c, gathered[c], results[c], me)
        if lending and c == 2:
            pl.when(me < 2)(back_copy(1, far[0]).start)
            pl.when(me == 0)(back_copy(1, near[1]).start)
        for d in peers():
            if lending and c in (1, 2) and d is near[0]:
                pl.when(jnp.logical_not(defers))(back_copy(c, d).start)
            elif lending and c == 1 and d is not near[0]:
                pl.when(me > 1 if d is far[0] else me != 0)(back_copy(c, d).start)
            else:
                back_copy(c, d).start()
        if lending and c == 2:

            @pl.when(helps)
            def _():
                with jax.named_scope("lent"):
                    bytes_of(lent_in, lent_sem).wait_recv()
                azimuth(full, lent_in, lent_out, 0)
                for d in (far[0], near[1]):
                    give_back(d).start()

        if c == 0:

            @pl.when(lowers)
            def _():
                pl.semaphore_wait(tied, 1)

            @pl.when(leads)
            def _():
                for d in peers():
                    pl.semaphore_signal(told, inc=1, device_id=(d, ring), device_id_type=MESH)

    if lending:

        @pl.when(keeps)
        def _():
            arrive(full)
            azimuth(full, gathered[full], results[full], me)
            for d in peers():
                if d is near[0]:
                    pl.when(jnp.logical_not(defers))(back_copy(full, d).start)
                else:
                    back_copy(full, d).start()

        @pl.when(defers)
        def _():
            for c in (*(1, 2), full):
                back_copy(c, near[0]).start()

        pl.when(helps)(give_back(near[0]).start)

    @pl.when(jnp.logical_not(leads))
    def _():
        pl.semaphore_wait(told, 1)

    def edge_ghost(d):
        down = d < 2
        row = 2 + base(True, d)
        target = jnp.where(down, rows + 2 + d, d - 2)
        beside = jnp.clip(ring + jnp.where(down, -1, 1), 0, rings - 1)
        copy = remote(
            landed.at[:, pl.ds(row, 1)], landed.at[:, pl.ds(target, 1)], ghost_send, ghost_recv, (me, beside)
        )
        pl.when(jnp.where(down, ring, rings - 1 - ring) > 0)(copy.start)

    if lending:
        edge_ghost(me)
        for k, d in enumerate(near + far):
            with jax.named_scope("edge%d" % k):
                bytes_of(results[0].at[0], edge_sems[k]).wait_recv()
            edge_ghost(d)
    else:
        for c in range(edges):
            home(c)
        for there, row, target, step in ((below, 2, rows + 2, -1), (above, rows, 0, 1)):
            beside = jnp.clip(ring + step, 0, rings - 1)
            copy = remote(
                landed.at[:, pl.ds(row, 2)], landed.at[:, pl.ds(target, 2)], ghost_send, ghost_recv, (me, beside)
            )
            pl.when(there)(copy.start)

    def advance(low_field, fields_in, spans):
        for f in range(low_field, low_field + fields_in):
            for low, high in spans:
                radial(landed, rate, bend, f, out, f, low, high)

    def ghosts_in():
        for case, received, _ in ghost_bytes:
            pl.when(case)(received.wait_recv)

    done = out.shape[0]
    if more and rows > 5:
        _, f0, n = chunks[1]
        home(1)
        advance(f0, n, [(2, rows - 2)])
        ghosts_in()
        advance(f0, n, [(0, 2), (rows - 2, rows)])
        for c in range(2, count):
            _, f0, n = chunks[c]
            home(c)
            if f0 < done:
                advance(f0, n, [(0, rows)])
    else:
        for c in range(edges, count):
            home(c)
        ghosts_in()
        advance(0, done, [(0, rows)])

    for c in range(full):
        bytes_of(boxes[c].at[pl.ds(0, 2 * (group - 1))], sent.at[c]).wait_send()
    if lending:
        for who, pieces in ((jnp.logical_not(keeps), 4), (helps, 8), (usual, 6)):
            pl.when(who)(bytes_of(lent.at[pl.ds(0, pieces)], sent.at[full]).wait_send)
    for case, _, delivered in ghost_bytes:
        pl.when(case)(delivered.wait_send)


def shards(fields, shift, fraction, radial_rate):
    nf, rows, polar, width = fields.shape
    group, rings = lax.axis_size("az"), lax.axis_size("rad")
    chunks = chunks_of(nf, rows, group)
    more = rows // group - 1
    boxes = [
        pltpu.VMEM((2 * group, n, 1 if first else more, polar, width), jnp.float32)
        for first, f0, n in chunks
    ]
    count = len(chunks)
    dma = pltpu.SemaphoreType.DMA
    lent = []
    if lends(rows, group):
        lent = [pltpu.VMEM((2 * group, 1, more, polar, width), jnp.float32), dma]
    operands = (fields, shift, fraction, radial_rate.T)
    left = chunks[-1][2]

    def like(*shape):
        return jax.ShapeDtypeStruct((*shape, polar, width), jnp.float32)

    vmem, hbm = pl.BlockSpec(memory_space=pltpu.VMEM), pl.BlockSpec(memory_space=pltpu.HBM)
    moved = pl.pallas_call(
        functools.partial(kernel, group, rings, chunks),
        out_shape=[like(nf - left, rows), like(nf, rows + 4), like(rows + 1), like(rows + 1)],
        in_specs=[hbm] * 4,
        out_specs=[vmem] * 4,
        scratch_shapes=[
            pltpu.SMEM(shift.shape, jnp.int32),
            pltpu.SMEM(fraction.shape, jnp.float32),
            pltpu.VMEM(radial_rate.shape[::-1], jnp.float32),
            *boxes,
            dma((3,)),
            dma((count,)),
            dma((count,)),
            dma((count + 2 * lends(rows, group),)),
            dma,
            dma,
            *[pltpu.SemaphoreType.REGULAR] * 3,
            *lent,
        ],
        compiler_params=pltpu.CompilerParams(
            collective_id=0, has_side_effects=True, vmem_limit_bytes=10 * fields.size * 4
        ),
    )(*(pltpu.with_memory_space_constraint(x, pltpu.HBM) for x in operands))
    return pl.pallas_call(
        finish,
        out_shape=jax.ShapeDtypeStruct(fields.shape, jnp.float32),
        in_specs=[vmem] * 4,
        out_specs=hbm,
        scratch_shapes=[pltpu.VMEM((left, rows, polar, width), jnp.float32), dma((2,))],
        compiler_params=pltpu.CompilerParams(vmem_limit_bytes=5 * fields.size * 4),
    )(*moved)


def solution(mesh):
    placed = (P(None, "rad", None, "az"), P(), P(), P())
    return jax.shard_map(
        shards, mesh=mesh, in_specs=placed, out_specs=P(None, "rad", None, "az"), check_vma=False
    )
```

```python
import functools

import jax
import jax.numpy as jnp
from jax import lax
from jax.experimental import pallas as pl
from jax.experimental.pallas import tpu as pltpu
from jax.sharding import PartitionSpec as P

MESH = pl.DeviceIdType.MESH


def half_slope(left, right):
    low = jnp.maximum(jnp.minimum(left, right), 0.0)
    high = jnp.minimum(jnp.maximum(left, right), 0.0)
    return jnp.maximum(jnp.minimum(0.25 * (left + right), low), high)


def chunks_of(fields, rows, group):
    rest = rows // group - 1
    if rest == 0:
        return [(True, f, 1) for f in range(fields)]
    if lends(rows, group):
        return [(True, 0, fields), (False, 0, fields - 2), (False, fields - 2, 1), (False, fields - 1, 1)]
    return [(True, 0, fields), (False, 0, fields - 2), (False, fields - 2, 2)]


def lends(rows, group):
    return group == 4 and rows > group


def radial(landed, rate, bend, f, target, g, low, high):
    q1, q2 = landed[f, low + 1], landed[f, low + 2]
    d1 = q1 - landed[f, low]
    d2 = q2 - q1
    h1 = half_slope(d1, d2)
    inner = None
    for j in range(low, high + 1):
        q3 = landed[f, j + 3]
        d3 = q3 - q2
        h2 = half_slope(d2, d3)
        c, b = rate[j], bend[j]
        ahead = c > 0.0
        flux = c * jnp.where(ahead, q1, q2) + b * jnp.where(ahead, h1, h2)
        if j > low:
            target[g, j - 1] = q1 - (flux - inner)
        inner = flux
        q1, q2, d2, h1 = q2, q3, d3, h2


def finish(done, landed, rate, bend, out, fresh, sems):
    ready = done.shape[0]
    early = pltpu.make_async_copy(done, out.at[pl.ds(0, ready)], sems.at[0])
    late = pltpu.make_async_copy(fresh, out.at[pl.ds(ready, fresh.shape[0])], sems.at[1])
    early.start()
    for g in range(fresh.shape[0]):
        radial(landed, rate, bend, ready + g, fresh, g, 0, fresh.shape[1])
    late.start()
    early.wait()
    late.wait()


def peers_of(group, me):
    if group == 4:
        inner = me + 1 - 2 * lax.rem(me, 2)
        outer = lax.rem(me + 2, 4)
        return [inner, outer], [inner + outer - me]
    return [lax.rem(me + step, group) for step in range(1, group)], []


def kernel(
    group, rings, chunks,
    fields, shift_in, fraction_in, rates_in,
    out, landed, rate, bend,
    shift, fraction, rates, tally, *rest,
):
    count = len(chunks)
    boxes, rest = rest[:count], rest[count:]
    gathered = [box.at[pl.ds(0, group)] for box in boxes]
    results = [box.at[pl.ds(group, group)] for box in boxes]
    small_sem, sent, gather_sem, home_sem, ghost_send, ghost_recv, passed, told, tied, *rest = rest
    lending = lends(fields.shape[1], group)
    if lending:
        lent, lent_sem = rest
        lent_in, lent_out = lent.at[pl.ds(0, group)], lent.at[pl.ds(group, group)]
    nf, rows, polar, width = fields.shape
    me, ring = lax.axis_index("az"), lax.axis_index("rad")
    more = rows // group - 1
    start = ring * rows

    def base(first, d):
        if first:
            return jnp.where(d < 2, d, jnp.where(d < 4, rows - 4 + d, d - 2))
        return group - 2 + d * more

    def height(first):
        return 1 if first else more

    def block(c, d, lift=0):
        first, f0, n = chunks[c]
        return pl.ds(f0, n), pl.ds(lift + base(first, d), height(first))

    near, far = peers_of(group, me)
    barrier = pltpu.get_barrier_semaphore()
    between = jnp.logical_or(me == 1, me == 2)

    def greet():
        for d in near:
            pl.semaphore_signal(barrier, inc=1, device_id=(d, ring), device_id_type=MESH)

    if far:
        pl.when(me != 3)(greet)
    else:
        greet()

    below, above = ring > 0, ring < rings - 1
    leads = me == 0

    def tell(who, semaphore, step):
        @pl.when(who)
        def _():
            pl.semaphore_signal(semaphore, inc=1, device_id=(me, ring + step), device_id_type=MESH)

    lowers, lifts = jnp.logical_and(leads, below), jnp.logical_and(leads, above)
    tell(lifts, barrier, 1)

    lender = ring == 0
    keeps = jnp.logical_or(me != 0, jnp.logical_not(lender))
    helps = jnp.logical_and(me == 3, lender)
    usual = jnp.logical_and(keeps, jnp.logical_not(helps))
    defers = jnp.logical_and(me > 1, lax.rem(ring, 2) == 0)

    def own_copy(c):
        return pltpu.make_async_copy(fields.at[block(c, me)], gathered[c].at[me], gather_sem.at[c])

    full = count - 1 if lending else count
    for c in range(full):
        own_copy(c).start()
    if lending:
        pl.when(keeps)(own_copy(full).start)

        @pl.when(helps)
        def _():
            pltpu.make_async_copy(fields.at[block(full, 0)], lent_in.at[me], lent_sem).start()

    small = [
        pltpu.make_async_copy(rates_in, rates, small_sem.at[0]),
        pltpu.make_async_copy(shift_in, shift, small_sem.at[1]),
        pltpu.make_async_copy(fraction_in, fraction, small_sem.at[2]),
    ]
    for copy in small:
        copy.start()

    with jax.named_scope("barrier"):
        greeted = jnp.where(between, 1, 2) if far else len(near)
        pl.semaphore_wait(barrier, greeted + jnp.where(lowers, 1, 0))
    if far:

        @pl.when(me == 3)
        def _():
            for d in near:
                pl.semaphore_signal(tied, inc=1, device_id=(d, ring), device_id_type=MESH)

    def remote(src, dst, send_sem, recv_sem, device):
        return pltpu.make_async_remote_copy(
            src_ref=src, dst_ref=dst, send_sem=send_sem, recv_sem=recv_sem,
            device_id=device, device_id_type=MESH,
        )

    def out_copy(c, d):
        return remote(fields.at[block(c, d)], gathered[c].at[me], sent, gather_sem.at[c], (d, ring))

    edge_sems = [home_sem.at[i] for i in (0, count, count + 1)] if lending else []

    def back_copy(c, d):
        landing = home_sem.at[c]
        if lending and c == 0:
            landing = edge_sems[[d is other for other in near + far].index(True)]
        return remote(results[c].at[d], landed.at[block(c, me, 2)], sent, landing, (d, ring))

    def lend():
        return remote(fields.at[block(full, 0)], lent_in.at[me], sent, lent_sem, (3, ring))

    def give_back(d):
        return remote(lent_out.at[d], landed.at[block(full, 0, 2)], sent, home_sem.at[full], (d, ring))

    def bytes_of(ref, semaphore):
        return remote(ref, ref, semaphore, semaphore, (me, ring))

    def arrive(c):
        with jax.named_scope("arrived"):
            bytes_of(gathered[c], gather_sem.at[c]).wait_recv()

    def home(c):
        with jax.named_scope("home"):
            if c < full:
                bytes_of(results[c].at[pl.ds(0, group - 1)], home_sem.at[c]).wait_recv()
                return
            for who, pieces in ((jnp.logical_not(keeps), 4), (helps, 2), (usual, 3)):
                pl.when(who)(bytes_of(results[c].at[pl.ds(0, pieces)], home_sem.at[c]).wait_recv)

    def peers():
        return far + near

    if far:
        known = [jnp.logical_or(jnp.logical_not(between), me == k + 1) for k in range(2)]
        for k in range(2):
            pl.when(known[k])(out_copy(0, near[k]).start)

        @pl.when(between)
        def _():
            with jax.named_scope("answer"):
                pl.semaphore_wait(tied, 1)
            for k in range(2):
                pl.when(me != k + 1)(out_copy(0, near[k]).start)

        pl.semaphore_signal(passed, inc=1, device_id=(near[0], ring), device_id_type=MESH)
        with jax.named_scope("passed"):
            pl.semaphore_wait(passed, 1)
    else:
        for d in near:
            out_copy(0, d).start()
    tell(lowers, told, -1)
    for c in range(full):
        for d in far + near if c else far:
            out_copy(c, d).start()
        if lending and c == 1:
            pl.when(jnp.logical_and(lender, me != 3))(lend().start)
    if lending:
        for d in far + near:
            pl.when(jnp.logical_or(d != 0, jnp.logical_not(lender)))(out_copy(full, d).start)

    small[0].wait()
    table = rates[...]
    place = lax.broadcasted_iota(jnp.int32, table.shape, 1)
    for j in range(rows + 1):
        column = jnp.sum(
            jnp.where(place == start - 1 + j, table, 0.0), axis=1, keepdims=True
        )
        if j == 0:
            column = jnp.where(ring > 0, column, 0.0)
        if j == rows:
            column = jnp.where(ring < rings - 1, column, 0.0)
        spread = jnp.broadcast_to(column, (polar, width))
        size = jnp.abs(spread)
        rate[j] = spread
        bend[j] = size * (1.0 - size)

    @pl.when(ring == 0)
    def _():
        landed[:, 0:2] = jnp.zeros((nf, 2, polar, width), jnp.float32)

    @pl.when(ring == rings - 1)
    def _():
        landed[:, rows + 2 : rows + 4] = jnp.zeros((nf, 2, polar, width), jnp.float32)

    lane = lax.broadcasted_iota(jnp.int32, (polar, width), 1)
    at_first, at_last = lane == 0, lane == width - 1

    def previous(blocks):
        turned = [pltpu.roll(b, 1, 1) for b in blocks]
        return [jnp.where(at_first, turned[p - 1], turned[p]) for p in range(group)]

    def following(blocks):
        turned = [pltpu.roll(b, width - 1, 1) for b in blocks]
        return [jnp.where(at_last, turned[(p + 1) % group], turned[p]) for p in range(group)]

    cycle = group * width

    def azimuth(c, source, target, owner):
        first, f0, n = chunks[c]
        for k in range(height(first)):
            row = start + base(first, owner) + k
            courant = fraction[row]
            ahead = courant > 0.0
            amount = shift[row] + jnp.where(ahead, cycle, cycle - 1)
            whole = lax.rem(amount // width, group)
            part = lax.rem(amount, width)
            size = jnp.abs(courant)
            bent = size * (1.0 - size)
            beyond = lane >= part

            for f in range(n):
                turned = [
                    pltpu.roll(source[lax.rem(p + group - whole, group), f, k], part, 1)
                    for p in range(group)
                ]
                q = [jnp.where(beyond, turned[p], turned[p - 1]) for p in range(group)]
                before = previous(q)
                left = [x - y for x, y in zip(q, before)]
                right = following(left)
                value = [
                    courant * x + bent * half_slope(l, r) for x, l, r in zip(q, left, right)
                ]
                lower = previous(value)
                for p in range(group):
                    kept = jnp.where(ahead, q[p], before[p])
                    target[p, f, k] = kept - (value[p] - lower[p])
        landed[block(c, owner, 2)] = target[me]

    inside = jnp.logical_and(below, above)
    ghost_bytes = [
        (inside, bytes_of(landed.at[:, pl.ds(0, 4)], ghost_recv), bytes_of(landed.at[:, pl.ds(0, 4)], ghost_send)),
        (below != above, bytes_of(landed.at[:, pl.ds(0, 2)], ghost_recv), bytes_of(landed.at[:, pl.ds(0, 2)], ghost_send)),
    ]

    edges = 1 if more else count

    small[1].wait()
    small[2].wait()

    @pl.when(lifts)
    def _():
        pl.semaphore_wait(told, 1)

    tell(lifts, tied, 1)
    for c in range(full):
        arrive(c)
        with jax.named_scope("azimuth"):
            azimuth(c, gathered[c], results[c], me)
        if lending and c == 2:
            pl.when(me < 2)(back_copy(1, far[0]).start)
            pl.when(me == 0)(back_copy(1, near[1]).start)
        for d in peers():
            if lending and c in (1, 2) and d is near[0]:
                pl.when(jnp.logical_not(defers))(back_copy(c, d).start)
            elif lending and c == 1 and d is not near[0]:
                pl.when(me > 1 if d is far[0] else me != 0)(back_copy(c, d).start)
            else:
                back_copy(c, d).start()
        if lending and c == 2:

            @pl.when(helps)
            def _():
                with jax.named_scope("lent"):
                    bytes_of(lent_in, lent_sem).wait_recv()
                azimuth(full, lent_in, lent_out, 0)
                for d in (far[0], near[1]):
                    give_back(d).start()

        if c == 0:

            @pl.when(lowers)
            def _():
                pl.semaphore_wait(tied, 1)

            @pl.when(leads)
            def _():
                for d in peers():
                    pl.semaphore_signal(told, inc=1, device_id=(d, ring), device_id_type=MESH)

    if lending:

        @pl.when(keeps)
        def _():
            arrive(full)
            azimuth(full, gathered[full], results[full], me)
            for d in peers():
                if d is near[0]:
                    pl.when(jnp.logical_not(defers))(back_copy(full, d).start)
                else:
                    back_copy(full, d).start()

        @pl.when(defers)
        def _():
            for c in (*(1, 2), full):
                back_copy(c, near[0]).start()

        pl.when(helps)(give_back(near[0]).start)

    @pl.when(jnp.logical_not(leads))
    def _():
        pl.semaphore_wait(told, 1)

    def edge_ghost(d):
        down = d < 2
        row = 2 + base(True, d)
        target = jnp.where(down, rows + 2 + d, d - 2)
        beside = jnp.clip(ring + jnp.where(down, -1, 1), 0, rings - 1)
        copy = remote(
            landed.at[:, pl.ds(row, 1)], landed.at[:, pl.ds(target, 1)], ghost_send, ghost_recv, (me, beside)
        )
        pl.when(jnp.where(down, ring, rings - 1 - ring) > 0)(copy.start)

    if lending:
        edge_ghost(me)
        for k, d in enumerate(near + far):
            with jax.named_scope("edge%d" % k):
                bytes_of(results[0].at[0], edge_sems[k]).wait_recv()
            edge_ghost(d)
    else:
        for c in range(edges):
            home(c)
        for there, row, target, step in ((below, 2, rows + 2, -1), (above, rows, 0, 1)):
            beside = jnp.clip(ring + step, 0, rings - 1)
            copy = remote(
                landed.at[:, pl.ds(row, 2)], landed.at[:, pl.ds(target, 2)], ghost_send, ghost_recv, (me, beside)
            )
            pl.when(there)(copy.start)

    def advance(low_field, fields_in, spans):
        for f in range(low_field, low_field + fields_in):
            for low, high in spans:
                radial(landed, rate, bend, f, out, f, low, high)

    def ghosts_in():
        for case, received, _ in ghost_bytes:
            pl.when(case)(received.wait_recv)

    done = out.shape[0]
    if more and rows > 5:
        _, f0, n = chunks[1]
        home(1)
        advance(f0, n, [(2, rows - 2)])
        ghosts_in()
        advance(f0, n, [(0, 2), (rows - 2, rows)])
        for c in range(2, count):
            _, f0, n = chunks[c]
            home(c)
            if f0 < done:
                advance(f0, n, [(0, rows)])
    else:
        for c in range(edges, count):
            home(c)
        ghosts_in()
        advance(0, done, [(0, rows)])

    always = 2 * (group - 1) * sum(n * height(first) for first, _, n in chunks[:full])
    if lending:
        piece = chunks[full][2] * more
        for who, pieces in ((jnp.logical_not(keeps), 4), (helps, 8), (usual, 6)):
            pl.when(who)(bytes_of(tally.at[pl.ds(0, always + pieces * piece)], sent).wait_send)
    else:
        bytes_of(tally.at[pl.ds(0, always)], sent).wait_send()
    for case, _, delivered in ghost_bytes:
        pl.when(case)(delivered.wait_send)


def shards(fields, shift, fraction, radial_rate):
    nf, rows, polar, width = fields.shape
    group, rings = lax.axis_size("az"), lax.axis_size("rad")
    chunks = chunks_of(nf, rows, group)
    more = rows // group - 1
    boxes = [
        pltpu.VMEM((2 * group, n, 1 if first else more, polar, width), jnp.float32)
        for first, f0, n in chunks
    ]
    count = len(chunks)
    dma = pltpu.SemaphoreType.DMA
    lent = []
    if lends(rows, group):
        lent = [pltpu.VMEM((2 * group, 1, more, polar, width), jnp.float32), dma]
    operands = (fields, shift, fraction, radial_rate.T)
    left = chunks[-1][2]

    def like(*shape):
        return jax.ShapeDtypeStruct((*shape, polar, width), jnp.float32)

    vmem, hbm = pl.BlockSpec(memory_space=pltpu.VMEM), pl.BlockSpec(memory_space=pltpu.HBM)
    moved = pl.pallas_call(
        functools.partial(kernel, group, rings, chunks),
        out_shape=[like(nf - left, rows), like(nf, rows + 4), like(rows + 1), like(rows + 1)],
        in_specs=[hbm] * 4,
        out_specs=[vmem] * 4,
        scratch_shapes=[
            pltpu.SMEM(shift.shape, jnp.int32),
            pltpu.SMEM(fraction.shape, jnp.float32),
            pltpu.VMEM(radial_rate.shape[::-1], jnp.float32),
            pltpu.VMEM((2 * group * nf * (1 + more), polar, width), jnp.float32),
            *boxes,
            dma((3,)),
            dma,
            dma((count,)),
            dma((count + 2 * lends(rows, group),)),
            dma,
            dma,
            *[pltpu.SemaphoreType.REGULAR] * 3,
            *lent,
        ],
        compiler_params=pltpu.CompilerParams(
            collective_id=0, has_side_effects=True, vmem_limit_bytes=10 * fields.size * 4
        ),
    )(*(pltpu.with_memory_space_constraint(x, pltpu.HBM) for x in operands))
    return pl.pallas_call(
        finish,
        out_shape=jax.ShapeDtypeStruct(fields.shape, jnp.float32),
        in_specs=[vmem] * 4,
        out_specs=hbm,
        scratch_shapes=[pltpu.VMEM((left, rows, polar, width), jnp.float32), dma((2,))],
        compiler_params=pltpu.CompilerParams(vmem_limit_bytes=5 * fields.size * 4),
    )(*moved)


def solution(mesh):
    placed = (P(None, "rad", None, "az"), P(), P(), P())
    return jax.shard_map(
        shards, mesh=mesh, in_specs=placed, out_specs=P(None, "rad", None, "az"), check_vma=False
    )
```
